8 devices in a mesh: dp: 1 (over z), tp: 2 (over y), cp: 4 (over x, core).
Axes of the slice: x: 2, y: 2, z: 1, core: 2. Of those that a mesh axis runs over, the one named last changes fastest.
Arguments:
- hidden: bfloat16 [4096, 3072], P(('dp', 'cp'))
- positions: int32 [4096], P(('dp', 'cp'))
- ln_gain: bfloat16 [3072], replicated
- w_q: bfloat16 [3072, 3072], P(None, 'tp')
- w_k: bfloat16 [3072, 1024], P(None, 'tp')
- w_v: bfloat16 [3072, 1024], P(None, 'tp')
- w_o: bfloat16 [3072, 3072], P('tp')
- w_gate: bfloat16 [3072, 8192], P(None, 'tp')
- w_up: bfloat16 [3072, 8192], P(None, 'tp')
- w_down: bfloat16 [8192, 3072], P('tp')
Outputs:
- output 1: bfloat16 [4096, 3072], P(('dp', 'cp'))
- output 2: bfloat16 [4096, 8, 128], P(('dp', 'cp'), 'tp')
- output 3: bfloat16 [4096, 8, 128], P(('dp', 'cp'), 'tp')
All inputs are finite; a program needn't handle non-finite values.
Results may differ from the reference program's by a relative error of at most 0.0123478.
Values are sent between devices in bfloat16 or wider.
A program may use at most 1 GiB of HBM per device.

```python
import jax
import jax.numpy as jnp
from jax import lax

D_MODEL = 3072
HEADS = 24
KV_HEADS = 8
FF_DIM = 8192
HEAD_DIM = 128
ROPE_BASE = 4000000
TOKENS = 4096
LN_EPS = 1e-5
Q_BLOCK = min(64, TOKENS)


def layer_norm(hidden, ln_gain):
    hidden_f = hidden.astype(jnp.float32)
    row_mean = jnp.mean(hidden_f, axis=-1, keepdims=True)
    centered = hidden_f - row_mean
    row_var = jnp.mean(centered * centered, axis=-1, keepdims=True)
    return (centered * lax.rsqrt(row_var + LN_EPS) * ln_gain.astype(jnp.float32)).astype(jnp.bfloat16)


def rotary(proj, positions):
    half_dim = HEAD_DIM // 2
    inv_freq = 1.0 / (ROPE_BASE ** (jnp.arange(0, HEAD_DIM, 2, dtype=jnp.float32) / HEAD_DIM))
    angles = positions.astype(jnp.float32)[:, None] * inv_freq[None, :]
    bcast_shape = (proj.shape[0],) + (1,) * (proj.ndim - 2) + (half_dim,)
    cosine = jnp.cos(angles).reshape(bcast_shape)
    sine_val = jnp.sin(angles).reshape(bcast_shape)
    paired = proj.astype(jnp.float32).reshape(proj.shape[:-1] + (half_dim, 2))
    even_part = paired[..., 0]
    odd_part = paired[..., 1]
    rotated = jnp.stack([even_part * cosine - odd_part * sine_val, odd_part * cosine + even_part * sine_val], axis=-1)
    return rotated.reshape(proj.shape).astype(jnp.bfloat16)


def setup_inputs(seed: int = 0, part: int = 0) -> dict:
    base_key = jax.random.key(seed)
    part_keys = jax.random.split(jax.random.fold_in(base_key, part), 2)
    weight_keys = jax.random.split(base_key, 8)
    q_width = HEADS * HEAD_DIM
    kv_width = KV_HEADS * HEAD_DIM
    d_scale = D_MODEL ** -0.5
    hidden = jax.random.normal(part_keys[0], (TOKENS, D_MODEL), jnp.float32)
    pos_steps = jax.random.randint(part_keys[1], (TOKENS,), 1, 3, dtype=jnp.int32)
    positions = (jnp.cumsum(pos_steps, dtype=jnp.int32) - pos_steps[0]).astype(jnp.int32)
    ln_gain = 1.0 + 0.3 * jax.random.normal(weight_keys[0], (D_MODEL,), jnp.float32)
    w_q = (1.5 * d_scale) * jax.random.normal(weight_keys[1], (D_MODEL, q_width), jnp.float32)
    w_k = (1.5 * d_scale) * jax.random.normal(weight_keys[2], (D_MODEL, kv_width), jnp.float32)
    w_v = d_scale * jax.random.normal(weight_keys[3], (D_MODEL, kv_width), jnp.float32)
    w_o = (2.0 * q_width ** -0.5) * jax.random.normal(weight_keys[4], (q_width, D_MODEL), jnp.float32)
    w_gate = d_scale * jax.random.normal(weight_keys[5], (D_MODEL, FF_DIM), jnp.float32)
    w_up = d_scale * jax.random.normal(weight_keys[6], (D_MODEL, FF_DIM), jnp.float32)
    w_down = (FF_DIM ** -0.5) * jax.random.normal(weight_keys[7], (FF_DIM, D_MODEL), jnp.float32)
    return {
        'hidden': hidden.astype(jnp.bfloat16),
        'positions': positions,
        'ln_gain': ln_gain.astype(jnp.bfloat16),
        'w_q': w_q.astype(jnp.bfloat16),
        'w_k': w_k.astype(jnp.bfloat16),
        'w_v': w_v.astype(jnp.bfloat16),
        'w_o': w_o.astype(jnp.bfloat16),
        'w_gate': w_gate.astype(jnp.bfloat16),
        'w_up': w_up.astype(jnp.bfloat16),
        'w_down': w_down.astype(jnp.bfloat16),
    }


def reference(hidden, positions, ln_gain, w_q, w_k, w_v, w_o, w_gate, w_up, w_down):
    group_size = HEADS // KV_HEADS
    normed = layer_norm(hidden, ln_gain)
    q_proj = jnp.dot(normed, w_q, preferred_element_type=jnp.float32).astype(jnp.bfloat16)
    k_proj = jnp.dot(normed, w_k, preferred_element_type=jnp.float32).astype(jnp.bfloat16)
    v_cache = jnp.dot(normed, w_v, preferred_element_type=jnp.float32).astype(jnp.bfloat16).reshape(TOKENS, KV_HEADS, HEAD_DIM)
    q_rot = rotary(q_proj.reshape(TOKENS, KV_HEADS, group_size, HEAD_DIM), positions)
    k_cache = rotary(k_proj.reshape(TOKENS, KV_HEADS, HEAD_DIM), positions)
    k_float = k_cache.astype(jnp.float32)
    v_float = v_cache.astype(jnp.float32)
    key_pos = jnp.arange(TOKENS)
    score_scale = HEAD_DIM ** -0.5
    q_blocks = q_rot.reshape(TOKENS // Q_BLOCK, Q_BLOCK, KV_HEADS, group_size, HEAD_DIM)

    def attend_block(block_args):
        block_id, q_block = block_args
        scores = jnp.einsum('qkgd,tkd->qkgt', q_block.astype(jnp.float32), k_float) * score_scale
        query_pos = block_id * Q_BLOCK + jnp.arange(Q_BLOCK)
        allowed = key_pos[None, :] <= query_pos[:, None]
        scores = jnp.where(allowed[:, None, None, :], scores, -jnp.inf)
        row_max = jnp.max(scores, axis=-1, keepdims=True)
        weights = jnp.exp(scores - row_max)
        row_sum = jnp.sum(weights, axis=-1, keepdims=True)
        probs = weights.astype(jnp.bfloat16).astype(jnp.float32)
        numer = jnp.einsum('qkgt,tkd->qkgd', probs, v_float)
        return (numer / row_sum).astype(jnp.bfloat16)

    attn = lax.map(attend_block, (jnp.arange(TOKENS // Q_BLOCK), q_blocks))
    attn_flat = attn.reshape(TOKENS, HEADS * HEAD_DIM)
    attn_out = jnp.dot(attn_flat, w_o, preferred_element_type=jnp.float32)
    gate_proj = jnp.dot(normed, w_gate, preferred_element_type=jnp.float32).astype(jnp.bfloat16)
    up_proj = jnp.dot(normed, w_up, preferred_element_type=jnp.float32).astype(jnp.bfloat16)
    mlp_act = (jax.nn.silu(gate_proj.astype(jnp.float32)) * up_proj.astype(jnp.float32)).astype(jnp.bfloat16)
    mlp_out = jnp.dot(mlp_act, w_down, preferred_element_type=jnp.float32)
    hidden_out = (hidden.astype(jnp.float32) + attn_out + mlp_out).astype(jnp.bfloat16)
    return (hidden_out, k_cache, v_cache)
```

```python
import functools

import jax
import jax.numpy as jnp
from jax import lax
from jax.experimental import pallas as pl
from jax.experimental.pallas import tpu as pltpu
from jax.sharding import PartitionSpec as P


HEAD_DIM = 128
ROPE_BASE = 4000000
LN_EPS = 1e-5
CHUNK = 512
LOG2E = 1.4426950408889634
BF16 = jnp.bfloat16
F32 = jnp.float32


def cost(flops, bytes_accessed, transcendentals=0):
    return pl.CostEstimate(flops=int(flops), bytes_accessed=int(bytes_accessed), transcendentals=int(transcendentals))


def rotary_tables(positions):
    lane = jnp.arange(HEAD_DIM)
    exponent = ((lane // 2) * 2).astype(F32) / HEAD_DIM
    inv_freq = 1.0 / (ROPE_BASE ** exponent)
    angles = positions.astype(F32)[:, None] * inv_freq[None, :]
    sign = jnp.where(lane % 2 == 0, -1.0, 1.0).astype(F32)
    return jnp.cos(angles), jnp.sin(angles) * sign[None, :]


def rotate_head(head, cosine, sine):
    even = lax.broadcasted_iota(jnp.int32, head.shape, 1) % 2 == 0
    other = jnp.where(even, pltpu.roll(head, HEAD_DIM - 1, 1), pltpu.roll(head, 1, 1))
    return (head * cosine + other * sine).astype(BF16)


def norm_kv_kernel(x_ref, gain_ref, wk_ref, wv_ref, cos_ref, sin_ref, h_ref, kv_ref, k_ref, v_ref):
    x = x_ref[...].astype(F32)
    width = x.shape[1]
    mean = jnp.sum(x, axis=1, keepdims=True) * (1.0 / width)
    centered = x - mean
    var = jnp.sum(centered * centered, axis=1, keepdims=True) * (1.0 / width)
    h = (centered * lax.rsqrt(var + LN_EPS) * gain_ref[...].astype(F32)).astype(BF16)
    h_ref[...] = h
    k = jnp.dot(h_ref[...], wk_ref[...], preferred_element_type=F32).astype(BF16)
    v = jnp.dot(h_ref[...], wv_ref[...], preferred_element_type=F32).astype(BF16)
    v_ref[...] = v
    cosine, sine = cos_ref[...], sin_ref[...]
    for head in range(k.shape[1] // HEAD_DIM):
        cols = slice(head * HEAD_DIM, (head + 1) * HEAD_DIM)
        rotated = rotate_head(k[:, cols].astype(F32), cosine, sine)
        k_ref[:, cols] = rotated
        kv_ref[head, 0] = rotated
        for start in range(0, k.shape[0], HEAD_DIM):
            kv_ref[head, 1, start:start + HEAD_DIM, :] = v[start:start + HEAD_DIM, cols].T


def norm_kv(x, gain, wk, wv, cosine, sine):
    rows, width = x.shape
    kv = wk.shape[1]
    groups = kv // HEAD_DIM
    tile = 256
    return pl.pallas_call(
        norm_kv_kernel,
        grid=(rows // tile,),
        in_specs=[
            pl.BlockSpec((tile, width), lambda i: (i, 0)),
            pl.BlockSpec((1, width), lambda i: (0, 0)),
            pl.BlockSpec((width, kv), lambda i: (0, 0)),
            pl.BlockSpec((width, kv), lambda i: (0, 0)),
            pl.BlockSpec((tile, HEAD_DIM), lambda i: (i, 0)),
            pl.BlockSpec((tile, HEAD_DIM), lambda i: (i, 0)),
        ],
        out_specs=[
            pl.BlockSpec((tile, width), lambda i: (i, 0)),
            pl.BlockSpec((groups, 2, tile, HEAD_DIM), lambda i: (0, 0, i, 0)),
            pl.BlockSpec((tile, kv), lambda i: (i, 0)),
            pl.BlockSpec((tile, kv), lambda i: (i, 0)),
        ],
        out_shape=[
            jax.ShapeDtypeStruct((rows, width), BF16),
            jax.ShapeDtypeStruct((groups, 2, rows, HEAD_DIM), BF16),
            jax.ShapeDtypeStruct((rows, kv), BF16),
            jax.ShapeDtypeStruct((rows, kv), BF16),
        ],
        cost_estimate=cost(4 * rows * width * kv, 4 * rows * width + 4 * width * kv),
        name='norm_kv',
    )(x, gain.reshape(1, width), wk, wv, cosine, sine)


def q_kernel(h_ref, w_ref, cos_ref, sin_ref, q_ref):
    q = jnp.dot(h_ref[...], w_ref[...], preferred_element_type=F32).astype(BF16)
    cosine, sine = cos_ref[...], sin_ref[...]
    for head in range(q.shape[1] // HEAD_DIM):
        cols = slice(head * HEAD_DIM, (head + 1) * HEAD_DIM)
        q_ref[:, cols] = rotate_head(q[:, cols].astype(F32), cosine, sine)


def q_proj(h, wq, cosine, sine):
    rows, width = h.shape
    cols = wq.shape[1]
    tile = 256
    return pl.pallas_call(
        q_kernel,
        grid=(cols // tile,),
        in_specs=[
            pl.BlockSpec((rows, width), lambda i: (0, 0)),
            pl.BlockSpec((width, tile), lambda i: (0, i)),
            pl.BlockSpec((rows, HEAD_DIM), lambda i: (0, 0)),
            pl.BlockSpec((rows, HEAD_DIM), lambda i: (0, 0)),
        ],
        out_specs=pl.BlockSpec((rows, tile), lambda i: (0, i)),
        out_shape=jax.ShapeDtypeStruct((rows, cols), BF16),
        cost_estimate=cost(2 * rows * width * cols, 2 * rows * width + 2 * width * cols),
        name='q_proj',
    )(h, wq, cosine, sine)


def attend_kernel(base, tile, group, blocks, flags_ref, q_ref, *refs):
    sources = refs[:1 + sum(blocks)]
    o_ref, m_ref, l_ref, acc_ref, s0_ref, s1_ref = refs[1 + sum(blocks):]
    scale2 = (HEAD_DIM ** -0.5) * LOG2E
    step = pl.program_id(1)
    active = pl.program_id(0) < flags_ref[0]

    def scores(kv, keys, j, buffer, masked):
        q = q_ref[:, j * HEAD_DIM:(j + 1) * HEAD_DIM]
        top = None
        for start in range(0, keys, CHUNK):
            size = min(CHUNK, keys - start)
            s = lax.dot_general(kv[0, start:start + size, :], q, (((1,), (1,)), ((), ())), preferred_element_type=F32)
            if masked and start + size > keys - tile:
                key = lax.broadcasted_iota(jnp.int32, s.shape, 0) + start
                query = lax.broadcasted_iota(jnp.int32, s.shape, 1) + (keys - tile)
                s = jnp.where(key <= query, s, -jnp.inf)
            buffer[start:start + size, :] = s
            part = jnp.max(s.reshape(size // 8, 8, tile), axis=0)
            top = part if top is None else jnp.maximum(top, part)
        return top

    def block(full, keys, first, masked):
        items = [(kv, j) for kv in full for j in range(group)]
        buffers = (s0_ref, s1_ref)
        top8 = scores(items[0][0], keys, items[0][1], buffers[0], masked)
        for n, (kv, j) in enumerate(items):
            top = jnp.max(top8, axis=0, keepdims=True)
            if not first:
                old = m_ref[j]
                top = jnp.maximum(top, old)
            if n + 1 < len(items):
                top8 = scores(items[n + 1][0], keys, items[n + 1][1], buffers[(n + 1) % 2], masked)
            total = part = None
            for start in range(0, keys, CHUNK):
                size = min(CHUNK, keys - start)
                e = jnp.exp2((buffers[n % 2][start:start + size, :] - top) * scale2)
                e8 = jnp.sum(e.reshape(size // 8, 8, tile), axis=0)
                vt = jnp.concatenate([kv[1, at:at + HEAD_DIM, :] for at in range(start, start + size, HEAD_DIM)], axis=1)
                product = lax.dot_general(vt, e.astype(BF16), (((1,), (0,)), ((), ())), preferred_element_type=F32)
                total = e8 if total is None else total + e8
                part = product if part is None else part + product
            total = jnp.sum(total, axis=0, keepdims=True)
            if not first:
                factor = jnp.exp2((old - top) * scale2)
                total = total + l_ref[j] * factor
                part = part + acc_ref[j] * factor
            m_ref[j] = top
            l_ref[j] = total
            acc_ref[j] = part

    for n in range(pl.num_programs(1)):

        @pl.when(active & (step == n))
        def _():
            block(sources[:1], base + (n + 1) * tile, True, True)

    start = 1
    for flag, many in enumerate(blocks):
        full = sources[start:start + many]
        start += many

        @pl.when(active & (flags_ref[1 + flag] > 0))
        def _():
            block(full, full[0].shape[1], False, False)

    @pl.when(active)
    def _():
        for j in range(group):
            out = acc_ref[j] / l_ref[j]
            o_ref[:, j * HEAD_DIM:(j + 1) * HEAD_DIM] = out.T.astype(BF16)


def attend(flags, q, base, count, groups, sources, first_groups, blocks):
    keys = sources[0].shape[2]
    width = q.shape[1] // groups
    group = width // HEAD_DIM
    tile = 256
    first = base // tile

    def kv_spec(array, start):
        last = array.shape[0] - 1
        return pl.BlockSpec((None, 2, keys, HEAD_DIM), lambda g, i, f: (jnp.minimum(start + g, last), 0, 0, 0))

    grid_spec = pltpu.PrefetchScalarGridSpec(
        num_scalar_prefetch=1,
        grid=(groups, count // tile),
        in_specs=[pl.BlockSpec((tile, width), lambda g, i, f: (first + i, g))] + [kv_spec(*pair) for pair in zip(sources, first_groups)],
        out_specs=pl.BlockSpec((tile, width), lambda g, i, f: (i, g)),
        scratch_shapes=[
            pltpu.VMEM((group, 1, tile), F32),
            pltpu.VMEM((group, 1, tile), F32),
            pltpu.VMEM((group, HEAD_DIM, tile), F32),
            pltpu.VMEM((keys, tile), F32),
            pltpu.VMEM((keys, tile), F32),
        ],
    )
    return pl.pallas_call(
        functools.partial(attend_kernel, base, tile, group, blocks),
        grid_spec=grid_spec,
        out_shape=jax.ShapeDtypeStruct((count, q.shape[1]), BF16),
        cost_estimate=cost(10 * count * keys * q.shape[1], 4 * len(sources) * keys * groups * HEAD_DIM, 3 * count * keys * groups * group),
        name='attend',
    )(flags, q, *sources)


def gate_up_kernel(h_ref, wg_ref, wu_ref, a_ref):
    gate = jnp.dot(h_ref[...], wg_ref[...], preferred_element_type=F32).astype(BF16).astype(F32)
    up = jnp.dot(h_ref[...], wu_ref[...], preferred_element_type=F32).astype(BF16).astype(F32)
    a_ref[...] = (gate * jax.nn.sigmoid(gate) * up).astype(BF16)


def gate_up(h, wg, wu, first, rows):
    width, cols = wg.shape
    tile = 512
    index = first // rows
    weight_spec = pl.BlockSpec((width, tile), lambda i: (0, i))
    return pl.pallas_call(
        gate_up_kernel,
        grid=(cols // tile,),
        in_specs=[pl.BlockSpec((rows, width), lambda i: (index, 0)), weight_spec, weight_spec],
        out_specs=pl.BlockSpec((rows, tile), lambda i: (0, i)),
        out_shape=jax.ShapeDtypeStruct((rows, cols), BF16),
        cost_estimate=cost(4 * rows * width * cols, 2 * rows * (width + cols) + 4 * width * cols),
        name='gate_up',
    )(h, wg, wu)


def down_kernel(flags_ref, a_ref, o_ref, back_ref, wd_ref, wo_ref, out_ref, o2_ref):
    kept = o_ref.shape[1] - back_ref.shape[1]

    @pl.when(pl.program_id(0) == 0)
    def _():
        o2_ref[...] = o_ref[...]

        @pl.when(flags_ref[2] > 0)
        def _():
            o2_ref[:, kept:] = back_ref[...]

    total = jnp.dot(a_ref[...], wd_ref[...], preferred_element_type=F32)
    total += jnp.dot(o2_ref[...], wo_ref[...], preferred_element_type=F32)
    out_ref[...] = total.astype(BF16)


def down(flags, a, o, back, wd, wo, a_row, o_row, back_row, rows, col, cols):
    tile = 256
    start = col // tile
    grid_spec = pltpu.PrefetchScalarGridSpec(
        num_scalar_prefetch=1,
        grid=(cols // tile,),
        in_specs=[
            pl.BlockSpec((rows, a.shape[1]), lambda i, f: (a_row // rows, 0)),
            pl.BlockSpec((rows, o.shape[1]), lambda i, f: (o_row // rows, 0)),
            pl.BlockSpec((rows, back.shape[1]), lambda i, f: (back_row // rows, 0)),
            pl.BlockSpec((wd.shape[0], tile), lambda i, f: (0, start + i)),
            pl.BlockSpec((wo.shape[0], tile), lambda i, f: (0, start + i)),
        ],
        out_specs=pl.BlockSpec((rows, tile), lambda i, f: (0, i)),
        scratch_shapes=[pltpu.VMEM((rows, o.shape[1]), BF16)],
    )
    return pl.pallas_call(
        down_kernel,
        grid_spec=grid_spec,
        out_shape=jax.ShapeDtypeStruct((rows, cols), BF16),
        cost_estimate=cost(2 * rows * (wd.shape[0] + wo.shape[0]) * cols, 2 * cols * (wd.shape[0] + wo.shape[0])),
        name='down',
    )(flags, a, o, back, wd, wo)


def add_kernel(x_ref, mine_ref, other_ref, *refs):
    total = mine_ref[...].astype(F32) + other_ref[...].astype(F32)
    refs[-1][...] = (x_ref[...].astype(F32) + total).astype(BF16)


def add_chunk(x, mine, other, out, first, col):
    rows, cols = mine.shape
    tile = min(256, rows)
    index, start = first // tile, col // cols
    place = pl.BlockSpec((tile, cols), lambda i: (index + i, start))
    chunk = pl.BlockSpec((tile, cols), lambda i: (i, 0))
    args, specs, alias = [x, mine, other], [place, chunk, chunk], {}
    if out is not None:
        args, specs, alias = args + [out], specs + [pl.BlockSpec(memory_space=pl.ANY)], {3: 0}
    return pl.pallas_call(
        add_kernel,
        grid=(rows // tile,),
        in_specs=specs,
        out_specs=place,
        out_shape=jax.ShapeDtypeStruct(x.shape, BF16),
        input_output_aliases=alias,
        cost_estimate=cost(3 * rows * cols, 8 * rows * cols),
        name='add',
    )(*args)


SCHEDULE = (
    ('mlp', 0, 512),
    ('moved', 0, 512),
    ('own', 0, 256),
    ('down', 0, 256, 0, 3072),
    ('own', 256, 256),
    ('down', 256, 256, 0, 3072),
    ('mlp', 512, 512),
    ('moved', 512, 512),
    ('own', 512, 256),
    ('down', 512, 256, 0, 3072),
    ('own', 768, 256),
    ('down', 768, 256, 0, 1536),
    ('down', 768, 256, 1536, 1536),
)


def solution(mesh):
    if mesh.shape['cp'] != 4 or mesh.shape['tp'] != 2:
        raise ValueError('mesh')

    def local_layer(hidden, positions, ln_gain, w_q, w_k, w_v, w_o, w_gate, w_up, w_down):
        me = lax.axis_index('cp')
        late = me // 2
        cosine, sine = rotary_tables(positions)
        normed, kv_own, k_own, v_own = norm_kv(hidden, ln_gain, w_k, w_v, cosine, sine)
        groups = kv_own.shape[0]
        keep = groups - 1
        send = functools.partial(lax.ppermute, axis_name='cp')
        kv_b = send(kv_own[:keep], perm=[(0, 2), (1, 3)])
        kv_a = send(kv_own, perm=[(0, 1), (1, 0), (2, 3)])
        kv_d = send(kv_own[keep:], perm=[(3, 0), (2, 1)])
        kv_e = send(kv_own[keep:], perm=[(2, 0)])
        kv_c = send(kv_b, perm=[(2, 3), (3, 2)])
        own_flags = jnp.stack([groups - late, me % 2, late]).astype(jnp.int32)
        moved_flags = jnp.stack([1 - late, 1 - late, (me == 0).astype(jnp.int32)]).astype(jnp.int32)
        q_rot = q_proj(normed, w_q, cosine, sine)
        moved_width = q_rot.shape[1] // groups
        q_moved = send(q_rot[:, keep * moved_width:], perm=[(3, 0), (2, 1)])
        last = q_rot
        acts, backs, attns, pieces = [], [], [], []
        for kind, first, rows, *place in SCHEDULE:
            if kind == 'mlp':
                normed, last = lax.optimization_barrier((normed, last))
                last = gate_up(normed, w_gate, w_up, first, rows)
                acts.append((first, last))
            if kind == 'moved':
                q_moved, last = lax.optimization_barrier((q_moved, last))
                sources = (kv_d, kv_own, kv_a, kv_e)
                last = attend(moved_flags, q_moved, first, rows, 1, sources, (0, keep, keep, 0), (2, 1))
                backs.append((first, send(last, perm=[(0, 3), (1, 2)])))
            if kind == 'own':
                q_rot, last = lax.optimization_barrier((q_rot, last))
                sources = (kv_own, kv_a, kv_b, kv_c)
                last = attend(own_flags, q_rot, first, rows, groups, sources, (0, 0, 0, 0), (1, 2))
                attns.append((first, last))
            if kind == 'down':
                col, cols = place
                (a_first, act), (o_first, attn), (b_first, back) = [
                    [pair for pair in pairs if pair[0] <= first][-1] for pairs in (acts, attns, backs)
                ]
                act, last = lax.optimization_barrier((act, last))
                offsets = (first - a_first, first - o_first, first - b_first)
                last = down(own_flags, act, attn, back, w_down, w_o, *offsets, rows, col, cols)
                other = lax.ppermute(last, 'tp', [(0, 1), (1, 0)])
                pieces.append((last, other, first, col))
        k_own, v_own, last = lax.optimization_barrier((k_own, v_own, last))
        cache_shape = (k_own.shape[0], groups, HEAD_DIM)
        k_cache, v_cache = k_own.reshape(cache_shape), v_own.reshape(cache_shape)
        hidden_out = None
        for part, other, first, col in pieces:
            hidden_out = add_chunk(hidden, part, other, hidden_out, first, col)
        return hidden_out, k_cache, v_cache

    row_spec = P(('dp', 'cp'), None)
    col_spec = P(None, 'tp')
    cache_spec = P(('dp', 'cp'), 'tp', None)
    in_specs = (row_spec, P(('dp', 'cp')), P(None), col_spec, col_spec, col_spec, P('tp', None), col_spec, col_spec, P('tp', None))
    return jax.shard_map(local_layer, mesh=mesh, in_specs=in_specs, out_specs=(row_spec, cache_spec, cache_spec), check_vma=False)
```

```python
import functools

import jax
import jax.numpy as jnp
from jax import lax
from jax.experimental import pallas as pl
from jax.experimental.pallas import tpu as pltpu
from jax.sharding import PartitionSpec as P


HEAD_DIM = 128
ROPE_BASE = 4000000
LN_EPS = 1e-5
CHUNK = 512
LOG2E = 1.4426950408889634
BF16 = jnp.bfloat16
F32 = jnp.float32


def cost(flops, bytes_accessed, transcendentals=0):
    return pl.CostEstimate(flops=int(flops), bytes_accessed=int(bytes_accessed), transcendentals=int(transcendentals))


def rotary_tables(positions):
    lane = jnp.arange(HEAD_DIM)
    exponent = ((lane // 2) * 2).astype(F32) / HEAD_DIM
    inv_freq = 1.0 / (ROPE_BASE ** exponent)
    angles = positions.astype(F32)[:, None] * inv_freq[None, :]
    sign = jnp.where(lane % 2 == 0, -1.0, 1.0).astype(F32)
    return jnp.cos(angles), jnp.sin(angles) * sign[None, :]


def rotate_head(head, cosine, sine):
    even = lax.broadcasted_iota(jnp.int32, head.shape, 1) % 2 == 0
    other = jnp.where(even, pltpu.roll(head, HEAD_DIM - 1, 1), pltpu.roll(head, 1, 1))
    return (head * cosine + other * sine).astype(BF16)


def norm_kv_kernel(x_ref, gain_ref, wk_ref, wv_ref, cos_ref, sin_ref, h_ref, kv_ref, k_ref, v_ref):
    x = x_ref[...].astype(F32)
    width = x.shape[1]
    mean = jnp.sum(x, axis=1, keepdims=True) * (1.0 / width)
    centered = x - mean
    var = jnp.sum(centered * centered, axis=1, keepdims=True) * (1.0 / width)
    h = (centered * lax.rsqrt(var + LN_EPS) * gain_ref[...].astype(F32)[None, :]).astype(BF16)
    h_ref[...] = h
    k = jnp.dot(h_ref[...], wk_ref[...], preferred_element_type=F32).astype(BF16)
    v = jnp.dot(h_ref[...], wv_ref[...], preferred_element_type=F32).astype(BF16)
    v_ref[...] = v
    cosine, sine = cos_ref[...], sin_ref[...]
    for head in range(k.shape[1] // HEAD_DIM):
        cols = slice(head * HEAD_DIM, (head + 1) * HEAD_DIM)
        rotated = rotate_head(k[:, cols].astype(F32), cosine, sine)
        k_ref[:, cols] = rotated
        kv_ref[head, 0] = rotated
        for start in range(0, k.shape[0], HEAD_DIM):
            kv_ref[head, 1, start:start + HEAD_DIM, :] = v[start:start + HEAD_DIM, cols].T


def norm_kv(x, gain, wk, wv, cosine, sine):
    rows, width = x.shape
    kv = wk.shape[1]
    groups = kv // HEAD_DIM
    tile = 256
    return pl.pallas_call(
        norm_kv_kernel,
        grid=(rows // tile,),
        in_specs=[
            pl.BlockSpec((tile, width), lambda i: (i, 0)),
            pl.BlockSpec((width,), lambda i: (0,)),
            pl.BlockSpec((width, kv), lambda i: (0, 0)),
            pl.BlockSpec((width, kv), lambda i: (0, 0)),
            pl.BlockSpec((tile, HEAD_DIM), lambda i: (i, 0)),
            pl.BlockSpec((tile, HEAD_DIM), lambda i: (i, 0)),
        ],
        out_specs=[
            pl.BlockSpec((tile, width), lambda i: (i, 0)),
            pl.BlockSpec((groups, 2, tile, HEAD_DIM), lambda i: (0, 0, i, 0)),
            pl.BlockSpec((tile, kv), lambda i: (i, 0)),
            pl.BlockSpec((tile, kv), lambda i: (i, 0)),
        ],
        out_shape=[
            jax.ShapeDtypeStruct((rows, width), BF16),
            jax.ShapeDtypeStruct((groups, 2, rows, HEAD_DIM), BF16),
            jax.ShapeDtypeStruct((rows, kv), BF16),
            jax.ShapeDtypeStruct((rows, kv), BF16),
        ],
        cost_estimate=cost(4 * rows * width * kv, 4 * rows * width + 4 * width * kv),
        name='norm_kv',
    )(x, gain, wk, wv, cosine, sine)


def q_kernel(h_ref, w_ref, cos_ref, sin_ref, q_ref):
    q = jnp.dot(h_ref[...], w_ref[...], preferred_element_type=F32).astype(BF16)
    cosine, sine = cos_ref[...], sin_ref[...]
    for head in range(q.shape[1] // HEAD_DIM):
        cols = slice(head * HEAD_DIM, (head + 1) * HEAD_DIM)
        q_ref[:, cols] = rotate_head(q[:, cols].astype(F32), cosine, sine)


def q_proj(h, wq, cosine, sine):
    rows, width = h.shape
    cols = wq.shape[1]
    tile = 512
    return pl.pallas_call(
        q_kernel,
        grid=(cols // tile,),
        in_specs=[
            pl.BlockSpec((rows, width), lambda i: (0, 0)),
            pl.BlockSpec((width, tile), lambda i: (0, i)),
            pl.BlockSpec((rows, HEAD_DIM), lambda i: (0, 0)),
            pl.BlockSpec((rows, HEAD_DIM), lambda i: (0, 0)),
        ],
        out_specs=pl.BlockSpec((rows, tile), lambda i: (0, i)),
        out_shape=jax.ShapeDtypeStruct((rows, cols), BF16),
        cost_estimate=cost(2 * rows * width * cols, 2 * rows * width + 2 * width * cols),
        name='q_proj',
    )(h, wq, cosine, sine)


def attend_kernel(base, tile, group, blocks, flags_ref, q_ref, *refs):
    sources = refs[:1 + sum(blocks)]
    o_ref, m_ref, l_ref, acc_ref, s0_ref, s1_ref = refs[1 + sum(blocks):]
    scale2 = (HEAD_DIM ** -0.5) * LOG2E
    step = pl.program_id(1)

    def scores(kv, keys, j, buffer, masked):
        q = q_ref[:, j * HEAD_DIM:(j + 1) * HEAD_DIM]
        top = None
        for start in range(0, keys, CHUNK):
            size = min(CHUNK, keys - start)
            s = lax.dot_general(kv[0, start:start + size, :], q, (((1,), (1,)), ((), ())), preferred_element_type=F32)
            if masked and start + size > keys - tile:
                key = lax.broadcasted_iota(jnp.int32, s.shape, 0) + start
                query = lax.broadcasted_iota(jnp.int32, s.shape, 1) + (keys - tile)
                s = jnp.where(key <= query, s, -jnp.inf)
            buffer[start:start + size, :] = s
            part = jnp.max(s.reshape(size // 8, 8, tile), axis=0)
            top = part if top is None else jnp.maximum(top, part)
        return top

    def block(full, keys, first, masked):
        items = [(kv, j) for kv in full for j in range(group)]
        buffers = (s0_ref, s1_ref)
        top8 = scores(items[0][0], keys, items[0][1], buffers[0], masked)
        for n, (kv, j) in enumerate(items):
            top = jnp.max(top8, axis=0, keepdims=True)
            if not first:
                old = m_ref[j]
                top = jnp.maximum(top, old)
            if n + 1 < len(items):
                top8 = scores(items[n + 1][0], keys, items[n + 1][1], buffers[(n + 1) % 2], masked)
            total = part = None
            for start in range(0, keys, CHUNK):
                size = min(CHUNK, keys - start)
                e = jnp.exp2((buffers[n % 2][start:start + size, :] - top) * scale2)
                e8 = jnp.sum(e.reshape(size // 8, 8, tile), axis=0)
                vt = jnp.concatenate([kv[1, at:at + HEAD_DIM, :] for at in range(start, start + size, HEAD_DIM)], axis=1)
                product = lax.dot_general(vt, e.astype(BF16), (((1,), (0,)), ((), ())), preferred_element_type=F32)
                total = e8 if total is None else total + e8
                part = product if part is None else part + product
            total = jnp.sum(total, axis=0, keepdims=True)
            if not first:
                factor = jnp.exp2((old - top) * scale2)
                total = total + l_ref[j] * factor
                part = part + acc_ref[j] * factor
            m_ref[j] = top
            l_ref[j] = total
            acc_ref[j] = part

    for n in range(pl.num_programs(1)):

        @pl.when(step == n)
        def _():
            block(sources[:1], base + (n + 1) * tile, True, True)

    start = 1
    for flag, many in enumerate(blocks):
        full = sources[start:start + many]
        start += many

        @pl.when(flags_ref[flag] > 0)
        def _():
            block(full, full[0].shape[1], False, False)

    for j in range(group):
        out = acc_ref[j] / l_ref[j]
        o_ref[:, j * HEAD_DIM:(j + 1) * HEAD_DIM] = out.T.astype(BF16)


def attend(flags, q, base, count, groups, sources, blocks):
    keys = sources[0].shape[2]
    width = q.shape[1] // groups
    group = width // HEAD_DIM
    tile = 256
    first = base // tile

    kv_spec = pl.BlockSpec((None, 2, keys, HEAD_DIM), lambda g, i, f: (g, 0, 0, 0))
    grid_spec = pltpu.PrefetchScalarGridSpec(
        num_scalar_prefetch=1,
        grid=(groups, count // tile),
        in_specs=[pl.BlockSpec((tile, width), lambda g, i, f: (first + i, g))] + [kv_spec] * len(sources),
        out_specs=pl.BlockSpec((tile, width), lambda g, i, f: (i, g)),
        scratch_shapes=[
            pltpu.VMEM((group, 1, tile), F32),
            pltpu.VMEM((group, 1, tile), F32),
            pltpu.VMEM((group, HEAD_DIM, tile), F32),
            pltpu.VMEM((keys, tile), F32),
            pltpu.VMEM((keys, tile), F32),
        ],
    )
    return pl.pallas_call(
        functools.partial(attend_kernel, base, tile, group, blocks),
        grid_spec=grid_spec,
        out_shape=jax.ShapeDtypeStruct((count, q.shape[1]), BF16),
        cost_estimate=cost(10 * count * keys * q.shape[1], 4 * len(sources) * keys * groups * HEAD_DIM, 3 * count * keys * groups * group),
        name='attend',
    )(flags, q, *sources)


def gate_up_kernel(h_ref, wg_ref, wu_ref, a_ref):
    gate = jnp.dot(h_ref[...], wg_ref[...], preferred_element_type=F32).astype(BF16).astype(F32)
    up = jnp.dot(h_ref[...], wu_ref[...], preferred_element_type=F32).astype(BF16).astype(F32)
    a_ref[...] = (gate * jax.nn.sigmoid(gate) * up).astype(BF16)


def gate_up(h, wg, wu, first, rows):
    width, cols = wg.shape
    tile = 512
    index = first // rows
    weight_spec = pl.BlockSpec((width, tile), lambda i: (0, i))
    return pl.pallas_call(
        gate_up_kernel,
        grid=(cols // tile,),
        in_specs=[pl.BlockSpec((rows, width), lambda i: (index, 0)), weight_spec, weight_spec],
        out_specs=pl.BlockSpec((rows, tile), lambda i: (0, i)),
        out_shape=jax.ShapeDtypeStruct((rows, cols), BF16),
        cost_estimate=cost(4 * rows * width * cols, 2 * rows * (width + cols) + 4 * width * cols),
        name='gate_up',
    )(h, wg, wu)


def down_kernel(a_ref, o_ref, wd_ref, wo_ref, out_ref):
    total = jnp.dot(a_ref[...], wd_ref[...], preferred_element_type=F32)
    total += jnp.dot(o_ref[...], wo_ref[...], preferred_element_type=F32)
    out_ref[...] = total.astype(BF16)


def down(a, o, wd, wo, a_row, o_row, rows, col, cols):
    tile = 512
    start = col // tile
    return pl.pallas_call(
        down_kernel,
        grid=(cols // tile,),
        in_specs=[
            pl.BlockSpec((rows, a.shape[1]), lambda i: (a_row // rows, 0)),
            pl.BlockSpec((rows, o.shape[1]), lambda i: (o_row // rows, 0)),
            pl.BlockSpec((wd.shape[0], tile), lambda i: (0, start + i)),
            pl.BlockSpec((wo.shape[0], tile), lambda i: (0, start + i)),
        ],
        out_specs=pl.BlockSpec((rows, tile), lambda i: (0, i)),
        out_shape=jax.ShapeDtypeStruct((rows, cols), BF16),
        cost_estimate=cost(2 * rows * (wd.shape[0] + wo.shape[0]) * cols, 2 * cols * (wd.shape[0] + wo.shape[0])),
        name='down',
    )(a, o, wd, wo)


def add_kernel(x_ref, mine_ref, other_ref, *refs):
    total = mine_ref[...].astype(F32) + other_ref[...].astype(F32)
    refs[-1][...] = (x_ref[...].astype(F32) + total).astype(BF16)


def add_chunk(x, mine, other, out, first, col):
    rows, cols = mine.shape
    tile = min(256, rows)
    index, start = first // tile, col // cols
    place = pl.BlockSpec((tile, cols), lambda i: (index + i, start))
    chunk = pl.BlockSpec((tile, cols), lambda i: (i, 0))
    args, specs, alias = [x, mine, other], [place, chunk, chunk], {}
    if out is not None:
        args, specs, alias = args + [out], specs + [pl.BlockSpec(memory_space=pl.ANY)], {3: 0}
    return pl.pallas_call(
        add_kernel,
        grid=(rows // tile,),
        in_specs=specs,
        out_specs=place,
        out_shape=jax.ShapeDtypeStruct(x.shape, BF16),
        input_output_aliases=alias,
        cost_estimate=cost(3 * rows * cols, 8 * rows * cols),
        name='add',
    )(*args)


SCHEDULE = (
    ('mlp', 0, 512),
    ('own', 0, 256),
    ('down', 0, 256, 0, 3072),
    ('own', 256, 256),
    ('down', 256, 256, 0, 3072),
    ('mlp', 512, 512),
    ('own', 512, 256),
    ('down', 512, 256, 0, 3072),
    ('own', 768, 256),
    ('down', 768, 256, 0, 1536),
    ('down', 768, 256, 1536, 1536),
)


def solution(mesh):
    if mesh.shape['cp'] != 4 or mesh.shape['tp'] != 2:
        raise ValueError('mesh')

    def local_layer(hidden, positions, ln_gain, w_q, w_k, w_v, w_o, w_gate, w_up, w_down):
        me = lax.axis_index('cp')
        cosine, sine = rotary_tables(positions)
        normed, kv_own, k_own, v_own = norm_kv(hidden, ln_gain, w_k, w_v, cosine, sine)
        groups = kv_own.shape[0]
        send = functools.partial(lax.ppermute, axis_name='cp')
        kv_b = send(kv_own, perm=[(0, 2), (1, 3)])
        kv_a = send(kv_own, perm=[(0, 1), (2, 3)])
        kv_c = send(kv_b, perm=[(2, 3), (3, 2)])
        flags = jnp.stack([me % 2, me // 2]).astype(jnp.int32)
        q_rot = q_proj(normed, w_q, cosine, sine)
        last = q_rot
        acts, attns, pieces = [], [], []
        for kind, first, rows, *place in SCHEDULE:
            if kind == 'mlp':
                normed, last = lax.optimization_barrier((normed, last))
                last = gate_up(normed, w_gate, w_up, first, rows)
                acts.append((first, last))
            if kind == 'own':
                q_rot, last = lax.optimization_barrier((q_rot, last))
                sources = (kv_own, kv_a, kv_b, kv_c)
                last = attend(flags, q_rot, first, rows, groups, sources, (1, 2))
                attns.append((first, last))
            if kind == 'down':
                col, cols = place
                (a_first, act), (o_first, attn) = [[pair for pair in pairs if pair[0] <= first][-1] for pairs in (acts, attns)]
                act, last = lax.optimization_barrier((act, last))
                last = down(act, attn, w_down, w_o, first - a_first, first - o_first, rows, col, cols)
                other = lax.ppermute(last, 'tp', [(0, 1), (1, 0)])
                pieces.append((last, other, first, col))
        k_own, v_own, last = lax.optimization_barrier((k_own, v_own, last))
        cache_shape = (k_own.shape[0], groups, HEAD_DIM)
        k_cache, v_cache = k_own.reshape(cache_shape), v_own.reshape(cache_shape)
        hidden_out = None
        for part, other, first, col in pieces:
            hidden_out = add_chunk(hidden, part, other, hidden_out, first, col)
        return hidden_out, k_cache, v_cache

    row_spec = P(('dp', 'cp'), None)
    col_spec = P(None, 'tp')
    cache_spec = P(('dp', 'cp'), 'tp', None)
    in_specs = (row_spec, P(('dp', 'cp')), P(None), col_spec, col_spec, col_spec, P('tp', None), col_spec, col_spec, P('tp', None))
    return jax.shard_map(local_layer, mesh=mesh, in_specs=in_specs, out_specs=(row_spec, cache_spec, cache_spec), check_vma=False)
```

```python
import functools

import jax
import jax.numpy as jnp
from jax import lax
from jax.experimental import pallas as pl
from jax.experimental.pallas import tpu as pltpu
from jax.sharding import PartitionSpec as P


HEAD_DIM = 128
ROPE_BASE = 4000000
LN_EPS = 1e-5
STRIPS = 4
LOG2E = 1.4426950408889634
BF16 = jnp.bfloat16
F32 = jnp.float32


def cost(flops, bytes_accessed, transcendentals=0):
    return pl.CostEstimate(flops=int(flops), bytes_accessed=int(bytes_accessed), transcendentals=int(transcendentals))


def rotary_tables(positions):
    lane = jnp.arange(HEAD_DIM)
    exponent = ((lane // 2) * 2).astype(F32) / HEAD_DIM
    inv_freq = 1.0 / (ROPE_BASE ** exponent)
    angles = positions.astype(F32)[:, None] * inv_freq[None, :]
    sign = jnp.where(lane % 2 == 0, -1.0, 1.0).astype(F32)
    return jnp.cos(angles), jnp.sin(angles) * sign[None, :]


def rotate_head(head, cosine, sine):
    even = lax.broadcasted_iota(jnp.int32, head.shape, 1) % 2 == 0
    other = jnp.where(even, pltpu.roll(head, HEAD_DIM - 1, 1), pltpu.roll(head, 1, 1))
    return (head * cosine + other * sine).astype(BF16)


def norm_kv_kernel(x_ref, gain_ref, wk_ref, wv_ref, cos_ref, sin_ref, h_ref, kv_ref, k_ref, v_ref):
    width = x_ref.shape[1]
    gain = gain_ref[...].astype(F32)[None, :]

    def normalise(n, carry):
        rows = pl.ds(pl.multiple_of(n * 16, 16), 16)
        x = x_ref[rows, :].astype(F32)
        mean = jnp.sum(x, axis=1, keepdims=True) * (1.0 / width)
        centered = x - mean
        var = jnp.sum(centered * centered, axis=1, keepdims=True) * (1.0 / width)
        h_ref[rows, :] = (centered * lax.rsqrt(var + LN_EPS) * gain).astype(BF16)
        return carry

    lax.fori_loop(0, x_ref.shape[0] // 16, normalise, 0, unroll=STRIPS)
    k = jnp.dot(h_ref[...], wk_ref[...], preferred_element_type=F32).astype(BF16)
    v = jnp.dot(h_ref[...], wv_ref[...], preferred_element_type=F32).astype(BF16)
    v_ref[...] = v
    cosine, sine = cos_ref[...], sin_ref[...]
    for head in range(k.shape[1] // HEAD_DIM):
        cols = slice(head * HEAD_DIM, (head + 1) * HEAD_DIM)
        rotated = rotate_head(k[:, cols].astype(F32), cosine, sine)
        k_ref[:, cols] = rotated
        kv_ref[head, 0] = rotated
        for start in range(0, k.shape[0], HEAD_DIM):
            kv_ref[head, 1, start:start + HEAD_DIM, :] = v[start:start + HEAD_DIM, cols].T


def norm_kv(x, gain, wk, wv, cosine, sine):
    rows, width = x.shape
    kv = wk.shape[1]
    groups = kv // HEAD_DIM
    tile = 256
    return pl.pallas_call(
        norm_kv_kernel,
        grid=(rows // tile,),
        in_specs=[
            pl.BlockSpec((tile, width), lambda i: (i, 0)),
            pl.BlockSpec((width,), lambda i: (0,)),
            pl.BlockSpec((width, kv), lambda i: (0, 0)),
            pl.BlockSpec((width, kv), lambda i: (0, 0)),
            pl.BlockSpec((tile, HEAD_DIM), lambda i: (i, 0)),
            pl.BlockSpec((tile, HEAD_DIM), lambda i: (i, 0)),
        ],
        out_specs=[
            pl.BlockSpec((tile, width), lambda i: (i, 0)),
            pl.BlockSpec((groups, 2, tile, HEAD_DIM), lambda i: (0, 0, i, 0)),
            pl.BlockSpec((tile, kv), lambda i: (i, 0)),
            pl.BlockSpec((tile, kv), lambda i: (i, 0)),
        ],
        out_shape=[
            jax.ShapeDtypeStruct((rows, width), BF16),
            jax.ShapeDtypeStruct((groups, 2, rows, HEAD_DIM), BF16),
            jax.ShapeDtypeStruct((rows, kv), BF16),
            jax.ShapeDtypeStruct((rows, kv), BF16),
        ],
        cost_estimate=cost(4 * rows * width * kv, 4 * rows * width + 4 * width * kv),
        name='norm_kv',
    )(x, gain, wk, wv, cosine, sine)


def q_kernel(h_ref, w_ref, cos_ref, sin_ref, q_ref):
    for start in range(0, h_ref.shape[0], 512):
        rows = slice(start, start + 512)
        q = jnp.dot(h_ref[rows, :], w_ref[...], preferred_element_type=F32).astype(BF16)
        cosine, sine = cos_ref[rows, :], sin_ref[rows, :]
        for head in range(q.shape[1] // HEAD_DIM):
            cols = slice(head * HEAD_DIM, (head + 1) * HEAD_DIM)
            q_ref[rows, cols] = rotate_head(q[:, cols].astype(F32), cosine, sine)


def q_proj(h, wq, cosine, sine):
    rows, width = h.shape
    cols = wq.shape[1]
    tile = 512
    return pl.pallas_call(
        q_kernel,
        grid=(cols // tile,),
        in_specs=[
            pl.BlockSpec((rows, width), lambda i: (0, 0)),
            pl.BlockSpec((width, tile), lambda i: (0, i)),
            pl.BlockSpec((rows, HEAD_DIM), lambda i: (0, 0)),
            pl.BlockSpec((rows, HEAD_DIM), lambda i: (0, 0)),
        ],
        out_specs=pl.BlockSpec((rows, tile), lambda i: (0, i)),
        out_shape=jax.ShapeDtypeStruct((rows, cols), BF16),
        cost_estimate=cost(2 * rows * width * cols, 2 * rows * width + 2 * width * cols),
        name='q_proj',
    )(h, wq, cosine, sine)


def attend_kernel(base, tile, chunk, group, blocks, flags_ref, q_ref, *refs):
    sources = refs[:1 + sum(blocks)]
    o_ref, m_ref, l_ref, acc_ref, s0_ref, s1_ref = refs[1 + sum(blocks):]
    scale2 = (HEAD_DIM ** -0.5) * LOG2E
    step = pl.program_id(1)

    def scores(kv, keys, j, buffer, masked):
        q = q_ref[:, j * HEAD_DIM:(j + 1) * HEAD_DIM]
        top = None
        for start in range(0, keys, chunk):
            size = min(chunk, keys - start)
            s = lax.dot_general(kv[0, start:start + size, :], q, (((1,), (1,)), ((), ())), preferred_element_type=F32)
            if masked and start + size > keys - tile:
                key = lax.broadcasted_iota(jnp.int32, s.shape, 0) + start
                query = lax.broadcasted_iota(jnp.int32, s.shape, 1) + (keys - tile)
                s = jnp.where(key <= query, s, -jnp.inf)
            buffer[start:start + size, :] = s
            part = jnp.max(s.reshape(size // 8, 8, tile), axis=0)
            top = part if top is None else jnp.maximum(top, part)
        return top

    def block(full, keys, first, masked):
        items = [(kv, j) for kv in full for j in range(group)]
        buffers = (s0_ref, s1_ref)
        top8 = scores(items[0][0], keys, items[0][1], buffers[0], masked)
        for n, (kv, j) in enumerate(items):
            top = jnp.max(top8, axis=0, keepdims=True)
            if not first:
                old = m_ref[j]
                top = jnp.maximum(top, old)
            if n + 1 < len(items):
                top8 = scores(items[n + 1][0], keys, items[n + 1][1], buffers[(n + 1) % 2], masked)
            total = part = None
            for start in range(0, keys, chunk):
                size = min(chunk, keys - start)
                e = jnp.exp2((buffers[n % 2][start:start + size, :] - top) * scale2)
                e8 = jnp.sum(e.reshape(size // 8, 8, tile), axis=0)
                vt = jnp.concatenate([kv[1, at:at + HEAD_DIM, :] for at in range(start, start + size, HEAD_DIM)], axis=1)
                product = lax.dot_general(vt, e.astype(BF16), (((1,), (0,)), ((), ())), preferred_element_type=F32)
                total = e8 if total is None else total + e8
                part = product if part is None else part + product
            total = jnp.sum(total, axis=0, keepdims=True)
            if not first:
                factor = jnp.exp2((old - top) * scale2)
                total = total + l_ref[j] * factor
                part = part + acc_ref[j] * factor
            m_ref[j] = top
            l_ref[j] = total
            acc_ref[j] = part

    for n in range(pl.num_programs(1)):

        @pl.when(step == n)
        def _():
            block(sources[:1], base + (n + 1) * tile, True, True)

    start = 1
    for flag, many in enumerate(blocks):
        full = sources[start:start + many]
        start += many

        @pl.when(flags_ref[flag] > 0)
        def _():
            block(full, full[0].shape[1], False, False)

    for j in range(group):
        out = acc_ref[j] / l_ref[j]
        o_ref[:, j * HEAD_DIM:(j + 1) * HEAD_DIM] = out.T.astype(BF16)


def attend(flags, q, base, count, groups, sources, blocks, tile):
    keys = sources[0].shape[2]
    width = q.shape[1] // groups
    group = width // HEAD_DIM
    first = base // tile

    kv_spec = pl.BlockSpec((None, 2, keys, HEAD_DIM), lambda g, i, f: (g, 0, 0, 0))
    grid_spec = pltpu.PrefetchScalarGridSpec(
        num_scalar_prefetch=1,
        grid=(groups, count // tile),
        in_specs=[pl.BlockSpec((tile, width), lambda g, i, f: (first + i, g))] + [kv_spec] * len(sources),
        out_specs=pl.BlockSpec((tile, width), lambda g, i, f: (i, g)),
        scratch_shapes=[
            pltpu.VMEM((group, 1, tile), F32),
            pltpu.VMEM((group, 1, tile), F32),
            pltpu.VMEM((group, HEAD_DIM, tile), F32),
            pltpu.VMEM((keys, tile), F32),
            pltpu.VMEM((keys, tile), F32),
        ],
    )
    return pl.pallas_call(
        functools.partial(attend_kernel, base, tile, 512, group, blocks),
        grid_spec=grid_spec,
        out_shape=jax.ShapeDtypeStruct((count, q.shape[1]), BF16),
        cost_estimate=cost(10 * count * keys * q.shape[1], 4 * len(sources) * keys * groups * HEAD_DIM, 3 * count * keys * groups * group),
        name='attend',
    )(flags, q, *sources)


def gate_up_kernel(h_ref, wg_ref, wu_ref, a_ref):
    gate = jnp.dot(h_ref[...], wg_ref[...], preferred_element_type=F32).astype(BF16).astype(F32)
    up = jnp.dot(h_ref[...], wu_ref[...], preferred_element_type=F32).astype(BF16).astype(F32)
    a_ref[...] = (gate * jax.nn.sigmoid(gate) * up).astype(BF16)


def gate_up(h, wg, wu, first, rows, col, cols):
    width = wg.shape[0]
    tile = 512
    index, start = first // rows, col // tile
    weight_spec = pl.BlockSpec((width, tile), lambda i: (0, start + i))
    return pl.pallas_call(
        gate_up_kernel,
        grid=(cols // tile,),
        in_specs=[pl.BlockSpec((rows, width), lambda i: (index, 0)), weight_spec, weight_spec],
        out_specs=pl.BlockSpec((rows, tile), lambda i: (0, i)),
        out_shape=jax.ShapeDtypeStruct((rows, cols), BF16),
        cost_estimate=cost(4 * rows * width * cols, 2 * rows * (width + cols) + 4 * width * cols),
        name='gate_up',
    )(h, wg, wu)


def down_kernel(acts, attns, streams, *refs):
    a_refs, o_refs = refs[:acts], refs[acts:acts + attns]
    w_refs, wo_ref, out_ref = refs[acts + attns:acts + attns + streams], refs[-2], refs[-1]
    depth = w_refs[0].shape[0]
    rows = out_ref.shape[0] // attns
    a_parts = [a_ref.at[:, start:start + depth] for a_ref in a_refs for start in range(0, a_ref.shape[1], depth)]
    for n, o_ref in enumerate(o_refs):
        place = slice(n * rows, (n + 1) * rows)
        total = jnp.dot(o_ref[...], wo_ref[...], preferred_element_type=F32)
        for a_part, w_ref in zip(a_parts, w_refs):
            total += jnp.dot(a_part[place, :], w_ref[...], preferred_element_type=F32)
        out_ref[place, :] = total.astype(BF16)


def down(acts, attns, wd, wo, rows, col, cols):
    tile = 512
    start = col // tile
    streams = 4
    depth = wd.shape[0] // streams

    def act_spec(array, row):
        return pl.BlockSpec((rows, array.shape[1]), lambda i: (row // rows, 0))

    def stream_spec(n):
        return pl.BlockSpec((depth, tile), lambda i: (n, start + i))

    return pl.pallas_call(
        functools.partial(down_kernel, len(acts), len(attns), streams),
        grid=(cols // tile,),
        in_specs=[act_spec(*pair) for pair in acts]
        + [pl.BlockSpec(o.shape, lambda i: (0, 0)) for o in attns]
        + [stream_spec(n) for n in range(streams)]
        + [pl.BlockSpec((wo.shape[0], tile), lambda i: (0, start + i))],
        out_specs=pl.BlockSpec((rows, tile), lambda i: (0, i)),
        out_shape=jax.ShapeDtypeStruct((rows, cols), BF16),
        cost_estimate=cost(2 * rows * (wd.shape[0] + wo.shape[0]) * cols, 2 * cols * (wd.shape[0] + wo.shape[0])),
        name='down',
    )(*[array for array, _ in acts], *attns, *[wd] * streams, wo)


def add_kernel(x_ref, mine_ref, other_ref, *refs):
    total = mine_ref[...].astype(F32) + other_ref[...].astype(F32)
    refs[-1][...] = (x_ref[...].astype(F32) + total).astype(BF16)


def add_chunk(x, mine, other, out, first, col):
    rows, cols = mine.shape
    tile = 256
    index, start = first // tile, col // cols
    place = pl.BlockSpec((tile, cols), lambda i: (index + i, start))
    chunk = pl.BlockSpec((tile, cols), lambda i: (i, 0))
    args, specs, alias = [x, mine, other], [place, chunk, chunk], {}
    if out is not None:
        args, specs, alias = args + [out], specs + [pl.BlockSpec(memory_space=pl.ANY)], {3: 0}
    return pl.pallas_call(
        add_kernel,
        grid=(rows // tile,),
        in_specs=specs,
        out_specs=place,
        out_shape=jax.ShapeDtypeStruct(x.shape, BF16),
        input_output_aliases=alias,
        cost_estimate=cost(3 * rows * cols, 8 * rows * cols),
        name='add',
    )(*args)


SCHEDULE = (
    ('mlp', 0, 512, 0, 4096),
    ('mlp', 512, 512, 0, 1024),
    ('own', 0, 512, 512),
    ('down', 0, 512, 0, 1536),
    ('down', 0, 512, 1536, 1536),
    ('mlp', 512, 512, 1024, 3072),
    ('own', 512, 256, 256),
    ('down', 512, 256, 0, 3072),
    ('own', 768, 256, 256),
    ('down', 768, 256, 0, 1536),
    ('down', 768, 256, 1536, 1536),
)


def solution(mesh):
    if mesh.shape['cp'] != 4 or mesh.shape['tp'] != 2:
        raise ValueError('mesh')

    def local_layer(hidden, positions, ln_gain, w_q, w_k, w_v, w_o, w_gate, w_up, w_down):
        me = lax.axis_index('cp')
        cosine, sine = rotary_tables(positions)
        normed, kv_own, k_own, v_own = norm_kv(hidden, ln_gain, w_k, w_v, cosine, sine)
        groups = kv_own.shape[0]
        send = functools.partial(lax.ppermute, axis_name='cp')
        kv_b = send(kv_own, perm=[(0, 2), (1, 3)])
        kv_a = send(kv_own, perm=[(0, 1), (2, 3)])
        kv_c = send(kv_b, perm=[(2, 3), (3, 2)])
        flags = jnp.stack([me % 2, me // 2]).astype(jnp.int32)
        q_rot = q_proj(normed, w_q, cosine, sine)
        last = q_rot
        acts, attns, pieces = [], [], []
        for kind, first, rows, *place in SCHEDULE:
            if kind == 'mlp':
                normed, last = lax.optimization_barrier((normed, last))
                last = gate_up(normed, w_gate, w_up, first, rows, *place)
                acts.append((first, rows, last))
            if kind == 'own':
                q_rot, last = lax.optimization_barrier((q_rot, last))
                sources = (kv_own, kv_a, kv_b, kv_c)
                last = attend(flags, q_rot, first, rows, groups, sources, (1, 2), *place)
                attns.append((first, last))
            if kind == 'down':
                col, cols = place
                act = [(array, first - start) for start, many, array in acts if start <= first < start + many]
                attn = [array for start, array in attns if first <= start < first + rows]
                attn, last = lax.optimization_barrier((attn, last))
                last = down(act, attn, w_down, w_o, rows, col, cols)
                other = lax.ppermute(last, 'tp', [(0, 1), (1, 0)])
                pieces.append((last, other, first, col))
        k_own, v_own, last = lax.optimization_barrier((k_own, v_own, last))
        cache_shape = (k_own.shape[0], groups, HEAD_DIM)
        k_cache, v_cache = k_own.reshape(cache_shape), v_own.reshape(cache_shape)
        hidden_out = None
        for part, other, first, col in pieces:
            hidden_out = add_chunk(hidden, part, other, hidden_out, first, col)
        return hidden_out, k_cache, v_cache

    row_spec = P(('dp', 'cp'), None)
    col_spec = P(None, 'tp')
    cache_spec = P(('dp', 'cp'), 'tp', None)
    in_specs = (row_spec, P(('dp', 'cp')), P(None), col_spec, col_spec, col_spec, P('tp', None), col_spec, col_spec, P('tp', None))
    return jax.shard_map(local_layer, mesh=mesh, in_specs=in_specs, out_specs=(row_spec, cache_spec, cache_spec), check_vma=False)
```

```python
import functools

import jax
import jax.numpy as jnp
from jax import lax
from jax.experimental import pallas as pl
from jax.experimental.pallas import tpu as pltpu
from jax.sharding import PartitionSpec as P


HEAD_DIM = 128
ROPE_BASE = 4000000
LN_EPS = 1e-5
LOG2E = 1.4426950408889634
BF16 = jnp.bfloat16
F32 = jnp.float32


def cost(flops, bytes_accessed, transcendentals=0):
    return pl.CostEstimate(flops=int(flops), bytes_accessed=int(bytes_accessed), transcendentals=int(transcendentals))


def rotary_tables(positions):
    lane = jnp.arange(HEAD_DIM)
    exponent = ((lane // 2) * 2).astype(F32) / HEAD_DIM
    inv_freq = 1.0 / (ROPE_BASE ** exponent)
    angles = positions.astype(F32)[:, None] * inv_freq[None, :]
    sign = jnp.where(lane % 2 == 0, -1.0, 1.0).astype(F32)
    return jnp.cos(angles), jnp.sin(angles) * sign[None, :]


def rotate_head(head, cosine, sine):
    even = lax.broadcasted_iota(jnp.int32, head.shape, 1) % 2 == 0
    other = jnp.where(even, pltpu.roll(head, HEAD_DIM - 1, 1), pltpu.roll(head, 1, 1))
    return (head * cosine + other * sine).astype(BF16)


def norm_kv_kernel(x_ref, gain_ref, wk_ref, wv_ref, cos_ref, sin_ref, h_ref, kv_ref, k_ref, v_ref):
    x = x_ref[...].astype(F32)
    width = x.shape[1]
    mean = jnp.sum(x, axis=1, keepdims=True) * (1.0 / width)
    centered = x - mean
    var = jnp.sum(centered * centered, axis=1, keepdims=True) * (1.0 / width)
    h_ref[...] = (centered * lax.rsqrt(var + LN_EPS) * gain_ref[...].astype(F32)[None, :]).astype(BF16)
    k = jnp.dot(h_ref[...], wk_ref[...], preferred_element_type=F32).astype(BF16)
    v = jnp.dot(h_ref[...], wv_ref[...], preferred_element_type=F32).astype(BF16)
    v_ref[...] = v
    cosine, sine = cos_ref[...], sin_ref[...]
    for head in range(k.shape[1] // HEAD_DIM):
        cols = slice(head * HEAD_DIM, (head + 1) * HEAD_DIM)
        rotated = rotate_head(k[:, cols].astype(F32), cosine, sine)
        k_ref[:, cols] = rotated
        kv_ref[head, 0] = rotated
        for start in range(0, k.shape[0], HEAD_DIM):
            kv_ref[head, 1, start:start + HEAD_DIM, :] = v[start:start + HEAD_DIM, cols].T


def norm_kv(x, gain, wk, wv, cosine, sine):
    rows, width = x.shape
    kv = wk.shape[1]
    groups = kv // HEAD_DIM
    tile = 256
    return pl.pallas_call(
        norm_kv_kernel,
        grid=(rows // tile,),
        in_specs=[
            pl.BlockSpec((tile, width), lambda i: (i, 0)),
            pl.BlockSpec((width,), lambda i: (0,)),
            pl.BlockSpec((width, kv), lambda i: (0, 0)),
            pl.BlockSpec((width, kv), lambda i: (0, 0)),
            pl.BlockSpec((tile, HEAD_DIM), lambda i: (i, 0)),
            pl.BlockSpec((tile, HEAD_DIM), lambda i: (i, 0)),
        ],
        out_specs=[
            pl.BlockSpec((tile, width), lambda i: (i, 0)),
            pl.BlockSpec((groups, 2, tile, HEAD_DIM), lambda i: (0, 0, i, 0)),
            pl.BlockSpec((tile, kv), lambda i: (i, 0)),
            pl.BlockSpec((tile, kv), lambda i: (i, 0)),
        ],
        out_shape=[
            jax.ShapeDtypeStruct((rows, width), BF16),
            jax.ShapeDtypeStruct((groups, 2, rows, HEAD_DIM), BF16),
            jax.ShapeDtypeStruct((rows, kv), BF16),
            jax.ShapeDtypeStruct((rows, kv), BF16),
        ],
        cost_estimate=cost(4 * rows * width * kv, 4 * rows * width + 4 * width * kv),
        name='norm_kv',
    )(x, gain, wk, wv, cosine, sine)


def q_kernel(h_ref, w_ref, cos_ref, sin_ref, q_ref):
    for start in range(0, h_ref.shape[0], 512):
        rows = slice(start, start + 512)
        q = jnp.dot(h_ref[rows, :], w_ref[...], preferred_element_type=F32).astype(BF16)
        cosine, sine = cos_ref[rows, :], sin_ref[rows, :]
        for head in range(q.shape[1] // HEAD_DIM):
            cols = slice(head * HEAD_DIM, (head + 1) * HEAD_DIM)
            q_ref[rows, cols] = rotate_head(q[:, cols].astype(F32), cosine, sine)


def q_proj(h, wq, cosine, sine):
    rows, width = h.shape
    cols = wq.shape[1]
    tile = 512
    return pl.pallas_call(
        q_kernel,
        grid=(cols // tile,),
        in_specs=[
            pl.BlockSpec((rows, width), lambda i: (0, 0)),
            pl.BlockSpec((width, tile), lambda i: (0, i)),
            pl.BlockSpec((rows, HEAD_DIM), lambda i: (0, 0)),
            pl.BlockSpec((rows, HEAD_DIM), lambda i: (0, 0)),
        ],
        out_specs=pl.BlockSpec((rows, tile), lambda i: (0, i)),
        out_shape=jax.ShapeDtypeStruct((rows, cols), BF16),
        cost_estimate=cost(2 * rows * width * cols, 2 * rows * width + 2 * width * cols),
        name='q_proj',
    )(h, wq, cosine, sine)


def attend_kernel(base, tile, chunk, group, blocks, flags_ref, q_ref, *refs):
    sources = refs[:1 + sum(blocks)]
    o_ref, m_ref, l_ref, acc_ref, s0_ref, s1_ref = refs[1 + sum(blocks):]
    scale2 = (HEAD_DIM ** -0.5) * LOG2E
    step = pl.program_id(1)

    def scores(kv, keys, j, buffer, masked):
        q = q_ref[:, j * HEAD_DIM:(j + 1) * HEAD_DIM]
        top = None
        for start in range(0, keys, chunk):
            size = min(chunk, keys - start)
            s = lax.dot_general(kv[0, start:start + size, :], q, (((1,), (1,)), ((), ())), preferred_element_type=F32)
            if masked and start + size > keys - tile:
                key = lax.broadcasted_iota(jnp.int32, s.shape, 0) + start
                query = lax.broadcasted_iota(jnp.int32, s.shape, 1) + (keys - tile)
                s = jnp.where(key <= query, s, -jnp.inf)
            buffer[start:start + size, :] = s
            part = jnp.max(s.reshape(size // 8, 8, tile), axis=0)
            top = part if top is None else jnp.maximum(top, part)
        return top

    def block(full, keys, first, masked):
        items = [(kv, j) for kv in full for j in range(group)]
        buffers = (s0_ref, s1_ref)
        top8 = scores(items[0][0], keys, items[0][1], buffers[0], masked)
        for n, (kv, j) in enumerate(items):
            top = jnp.max(top8, axis=0, keepdims=True)
            if not first:
                old = m_ref[j]
                top = jnp.maximum(top, old)
            if n + 1 < len(items):
                top8 = scores(items[n + 1][0], keys, items[n + 1][1], buffers[(n + 1) % 2], masked)
            total = part = None
            for start in range(0, keys, chunk):
                size = min(chunk, keys - start)
                e = jnp.exp2((buffers[n % 2][start:start + size, :] - top) * scale2)
                e8 = jnp.sum(e.reshape(size // 8, 8, tile), axis=0)
                vt = jnp.concatenate([kv[1, at:at + HEAD_DIM, :] for at in range(start, start + size, HEAD_DIM)], axis=1)
                product = lax.dot_general(vt, e.astype(BF16), (((1,), (0,)), ((), ())), preferred_element_type=F32)
                total = e8 if total is None else total + e8
                part = product if part is None else part + product
            total = jnp.sum(total, axis=0, keepdims=True)
            if not first:
                factor = jnp.exp2((old - top) * scale2)
                total = total + l_ref[j] * factor
                part = part + acc_ref[j] * factor
            m_ref[j] = top
            l_ref[j] = total
            acc_ref[j] = part

    for n in range(pl.num_programs(1)):

        @pl.when(step == n)
        def _():
            block(sources[:1], base + (n + 1) * tile, True, True)

    start = 1
    for flag, many in enumerate(blocks):
        full = sources[start:start + many]
        start += many

        @pl.when(flags_ref[flag] > 0)
        def _():
            block(full, full[0].shape[1], False, False)

    for j in range(group):
        out = acc_ref[j] / l_ref[j]
        o_ref[:, j * HEAD_DIM:(j + 1) * HEAD_DIM] = out.T.astype(BF16)


def attend(flags, q, base, count, groups, sources, blocks, tile):
    keys = sources[0].shape[2]
    width = q.shape[1] // groups
    group = width // HEAD_DIM
    first = base // tile

    kv_spec = pl.BlockSpec((None, 2, keys, HEAD_DIM), lambda g, i, f: (g, 0, 0, 0))
    grid_spec = pltpu.PrefetchScalarGridSpec(
        num_scalar_prefetch=1,
        grid=(groups, count // tile),
        in_specs=[pl.BlockSpec((tile, width), lambda g, i, f: (first + i, g))] + [kv_spec] * len(sources),
        out_specs=pl.BlockSpec((tile, width), lambda g, i, f: (i, g)),
        scratch_shapes=[
            pltpu.VMEM((group, 1, tile), F32),
            pltpu.VMEM((group, 1, tile), F32),
            pltpu.VMEM((group, HEAD_DIM, tile), F32),
            pltpu.VMEM((keys, tile), F32),
            pltpu.VMEM((keys, tile), F32),
        ],
    )
    return pl.pallas_call(
        functools.partial(attend_kernel, base, tile, 512, group, blocks),
        grid_spec=grid_spec,
        out_shape=jax.ShapeDtypeStruct((count, q.shape[1]), BF16),
        cost_estimate=cost(10 * count * keys * q.shape[1], 4 * len(sources) * keys * groups * HEAD_DIM, 3 * count * keys * groups * group),
        name='attend',
    )(flags, q, *sources)


def gate_up_kernel(h_ref, wg_ref, wu_ref, a_ref):
    gate = jnp.dot(h_ref[...], wg_ref[...], preferred_element_type=F32).astype(BF16).astype(F32)
    up = jnp.dot(h_ref[...], wu_ref[...], preferred_element_type=F32).astype(BF16).astype(F32)
    a_ref[...] = (gate * jax.nn.sigmoid(gate) * up).astype(BF16)


def gate_up(h, wg, wu, first, rows, col, cols):
    width = wg.shape[0]
    tile = 512
    index, start = first // rows, col // tile
    weight_spec = pl.BlockSpec((width, tile), lambda i: (0, start + i))
    return pl.pallas_call(
        gate_up_kernel,
        grid=(cols // tile,),
        in_specs=[pl.BlockSpec((rows, width), lambda i: (index, 0)), weight_spec, weight_spec],
        out_specs=pl.BlockSpec((rows, tile), lambda i: (0, i)),
        out_shape=jax.ShapeDtypeStruct((rows, cols), BF16),
        cost_estimate=cost(4 * rows * width * cols, 2 * rows * (width + cols) + 4 * width * cols),
        name='gate_up',
    )(h, wg, wu)


def down_kernel(acts, attns, streams, *refs):
    a_refs, o_refs = refs[:acts], refs[acts:acts + attns]
    w_refs, wo_ref, out_ref = refs[acts + attns:acts + attns + streams], refs[-2], refs[-1]
    depth = w_refs[0].shape[0]
    rows = out_ref.shape[0] // attns
    a_parts = [a_ref.at[:, start:start + depth] for a_ref in a_refs for start in range(0, a_ref.shape[1], depth)]
    for n, o_ref in enumerate(o_refs):
        place = slice(n * rows, (n + 1) * rows)
        total = jnp.dot(o_ref[...], wo_ref[...], preferred_element_type=F32)
        for a_part, w_ref in zip(a_parts, w_refs):
            total += jnp.dot(a_part[place, :], w_ref[...], preferred_element_type=F32)
        out_ref[place, :] = total.astype(BF16)


def down(acts, attns, wd, wo, rows, col, cols):
    tile = 512
    start = col // tile
    streams = 1
    depth = wd.shape[0] // streams

    def act_spec(array, row):
        return pl.BlockSpec((rows, array.shape[1]), lambda i: (row // rows, 0))

    def stream_spec(n):
        return pl.BlockSpec((depth, tile), lambda i: (n, start + i))

    return pl.pallas_call(
        functools.partial(down_kernel, len(acts), len(attns), streams),
        grid=(cols // tile,),
        in_specs=[act_spec(*pair) for pair in acts]
        + [pl.BlockSpec(o.shape, lambda i: (0, 0)) for o in attns]
        + [stream_spec(n) for n in range(streams)]
        + [pl.BlockSpec((wo.shape[0], tile), lambda i: (0, start + i))],
        out_specs=pl.BlockSpec((rows, tile), lambda i: (0, i)),
        out_shape=jax.ShapeDtypeStruct((rows, cols), BF16),
        cost_estimate=cost(2 * rows * (wd.shape[0] + wo.shape[0]) * cols, 2 * cols * (wd.shape[0] + wo.shape[0])),
        name='down',
    )(*[array for array, _ in acts], *attns, *[wd] * streams, wo)


def add_kernel(x_ref, mine_ref, other_ref, *refs):
    total = mine_ref[...].astype(F32) + other_ref[...].astype(F32)
    refs[-1][...] = (x_ref[...].astype(F32) + total).astype(BF16)


def add_chunk(x, mine, other, out, first, col):
    rows, cols = mine.shape
    tile = 256
    index, start = first // tile, col // cols
    place = pl.BlockSpec((tile, cols), lambda i: (index + i, start))
    chunk = pl.BlockSpec((tile, cols), lambda i: (i, 0))
    args, specs, alias = [x, mine, other], [place, chunk, chunk], {}
    if out is not None:
        args, specs, alias = args + [out], specs + [pl.BlockSpec(memory_space=pl.ANY)], {3: 0}
    return pl.pallas_call(
        add_kernel,
        grid=(rows // tile,),
        in_specs=specs,
        out_specs=place,
        out_shape=jax.ShapeDtypeStruct(x.shape, BF16),
        input_output_aliases=alias,
        cost_estimate=cost(3 * rows * cols, 8 * rows * cols),
        name='add',
    )(*args)


SCHEDULE = (
    ('mlp', 0, 512, 0, 4096),
    ('own', 0, 512, 512),
    ('down', 0, 512, 0, 3072),
    ('mlp', 512, 512, 0, 4096),
    ('own', 512, 512, 512),
    ('down', 512, 512, 0, 1536),
    ('down', 512, 512, 1536, 1536),
)


def solution(mesh):
    if mesh.shape['cp'] != 4 or mesh.shape['tp'] != 2:
        raise ValueError('mesh')

    def local_layer(hidden, positions, ln_gain, w_q, w_k, w_v, w_o, w_gate, w_up, w_down):
        me = lax.axis_index('cp')
        cosine, sine = rotary_tables(positions)
        normed, kv_own, k_own, v_own = norm_kv(hidden, ln_gain, w_k, w_v, cosine, sine)
        groups = kv_own.shape[0]
        send = functools.partial(lax.ppermute, axis_name='cp')
        kv_b = send(kv_own, perm=[(0, 2), (1, 3)])
        kv_a = send(kv_own, perm=[(0, 1), (2, 3)])
        kv_c = send(kv_b, perm=[(2, 3), (3, 2)])
        cache_shape = (k_own.shape[0], groups, HEAD_DIM)
        k_cache, v_cache = k_own.reshape(cache_shape), v_own.reshape(cache_shape)
        flags = jnp.stack([me % 2, me // 2]).astype(jnp.int32)
        q_rot = q_proj(normed, w_q, cosine, sine)
        last = q_rot
        acts, attns, pieces = [], [], []
        for kind, first, rows, *place in SCHEDULE:
            if kind == 'mlp':
                normed, last = lax.optimization_barrier((normed, last))
                last = gate_up(normed, w_gate, w_up, first, rows, *place)
                acts.append((first, rows, last))
            if kind == 'own':
                q_rot, last = lax.optimization_barrier((q_rot, last))
                sources = (kv_own, kv_a, kv_b, kv_c)
                last = attend(flags, q_rot, first, rows, groups, sources, (1, 2), *place)
                attns.append((first, last))
            if kind == 'down':
                col, cols = place
                act = [(array, first - start) for start, many, array in acts if start <= first < start + many]
                attn = [array for start, array in attns if first <= start < first + rows]
                attn, last = lax.optimization_barrier((attn, last))
                last = down(act, attn, w_down, w_o, rows, col, cols)
                other = lax.ppermute(last, 'tp', [(0, 1), (1, 0)])
                pieces.append((last, other, first, col))
        hidden_out = None
        for part, other, first, col in pieces:
            hidden_out = add_chunk(hidden, part, other, hidden_out, first, col)
        return hidden_out, k_cache, v_cache

    row_spec = P(('dp', 'cp'), None)
    col_spec = P(None, 'tp')
    cache_spec = P(('dp', 'cp'), 'tp', None)
    in_specs = (row_spec, P(('dp', 'cp')), P(None), col_spec, col_spec, col_spec, P('tp', None), col_spec, col_spec, P('tp', None))
    return jax.shard_map(local_layer, mesh=mesh, in_specs=in_specs, out_specs=(row_spec, cache_spec, cache_spec), check_vma=False)
```

```python
import functools

import jax
import jax.numpy as jnp
from jax import lax
from jax.experimental import pallas as pl
from jax.experimental.pallas import tpu as pltpu
from jax.sharding import PartitionSpec as P


HEAD_DIM = 128
ROPE_BASE = 4000000
LN_EPS = 1e-5
LOG2E = 1.4426950408889634
BF16 = jnp.bfloat16
F32 = jnp.float32


def cost(flops, bytes_accessed, transcendentals=0):
    return pl.CostEstimate(flops=int(flops), bytes_accessed=int(bytes_accessed), transcendentals=int(transcendentals))


def rotary_tables(positions):
    lane = jnp.arange(HEAD_DIM)
    exponent = ((lane // 2) * 2).astype(F32) / HEAD_DIM
    inv_freq = 1.0 / (ROPE_BASE ** exponent)
    angles = positions.astype(F32)[:, None] * inv_freq[None, :]
    sign = jnp.where(lane % 2 == 0, -1.0, 1.0).astype(F32)
    return jnp.cos(angles), jnp.sin(angles) * sign[None, :]


def rotate_head(head, cosine, sine):
    even = lax.broadcasted_iota(jnp.int32, head.shape, 1) % 2 == 0
    other = jnp.where(even, pltpu.roll(head, HEAD_DIM - 1, 1), pltpu.roll(head, 1, 1))
    return (head * cosine + other * sine).astype(BF16)


def norm_kv_kernel(x_ref, gain_ref, wk_ref, wv_ref, cos_ref, sin_ref, h_ref, kv_ref, k_ref, v_ref, even_ref, odd_ref):
    step = pl.program_id(0)

    def body(made, used):
        k = jnp.dot(used[...], wk_ref[...], preferred_element_type=F32).astype(BF16)
        v = jnp.dot(used[...], wv_ref[...], preferred_element_type=F32).astype(BF16)
        x = x_ref[...].astype(F32)
        width = x.shape[1]
        mean = jnp.sum(x, axis=1, keepdims=True) * (1.0 / width)
        centered = x - mean
        var = jnp.sum(centered * centered, axis=1, keepdims=True) * (1.0 / width)
        h = (centered * lax.rsqrt(var + LN_EPS) * gain_ref[...].astype(F32)[None, :]).astype(BF16)
        made[...] = h
        h_ref[...] = h
        v_ref[...] = v
        cosine, sine = cos_ref[...], sin_ref[...]
        for head in range(k.shape[1] // HEAD_DIM):
            cols = slice(head * HEAD_DIM, (head + 1) * HEAD_DIM)
            rotated = rotate_head(k[:, cols].astype(F32), cosine, sine)
            k_ref[:, cols] = rotated
            kv_ref[head, 0] = rotated
            for start in range(0, k.shape[0], HEAD_DIM):
                kv_ref[head, 1, start:start + HEAD_DIM, :] = v[start:start + HEAD_DIM, cols].T

    @pl.when(step == 0)
    def _():
        odd_ref[...] = jnp.zeros_like(odd_ref)

    @pl.when(step % 2 == 0)
    def _():
        body(even_ref, odd_ref)

    @pl.when(step % 2 == 1)
    def _():
        body(odd_ref, even_ref)


def norm_kv(x, gain, wk, wv, cosine, sine):
    rows, width = x.shape
    kv = wk.shape[1]
    groups = kv // HEAD_DIM
    tile = 256
    tiles = rows // tile
    return pl.pallas_call(
        norm_kv_kernel,
        grid=(tiles + 1,),
        in_specs=[
            pl.BlockSpec((tile, width), lambda i: (jnp.minimum(i, tiles - 1), 0)),
            pl.BlockSpec((width,), lambda i: (0,)),
            pl.BlockSpec((width, kv), lambda i: (0, 0)),
            pl.BlockSpec((width, kv), lambda i: (0, 0)),
            pl.BlockSpec((tile, HEAD_DIM), lambda i: (jnp.maximum(i - 1, 0), 0)),
            pl.BlockSpec((tile, HEAD_DIM), lambda i: (jnp.maximum(i - 1, 0), 0)),
        ],
        out_specs=[
            pl.BlockSpec((tile, width), lambda i: (jnp.minimum(i, tiles - 1), 0)),
            pl.BlockSpec((groups, 2, tile, HEAD_DIM), lambda i: (0, 0, jnp.maximum(i - 1, 0), 0)),
            pl.BlockSpec((tile, kv), lambda i: (jnp.maximum(i - 1, 0), 0)),
            pl.BlockSpec((tile, kv), lambda i: (jnp.maximum(i - 1, 0), 0)),
        ],
        out_shape=[
            jax.ShapeDtypeStruct((rows, width), BF16),
            jax.ShapeDtypeStruct((groups, 2, rows, HEAD_DIM), BF16),
            jax.ShapeDtypeStruct((rows, kv), BF16),
            jax.ShapeDtypeStruct((rows, kv), BF16),
        ],
        scratch_shapes=[pltpu.VMEM((tile, width), BF16)] * 2,
        cost_estimate=cost(4 * rows * width * kv, 4 * rows * width + 4 * width * kv),
        name='norm_kv',
    )(x, gain, wk, wv, cosine, sine)


def q_kernel(h_ref, w_ref, cos_ref, sin_ref, q_ref):
    for start in range(0, h_ref.shape[0], 512):
        rows = slice(start, start + 512)
        q = jnp.dot(h_ref[rows, :], w_ref[...], preferred_element_type=F32).astype(BF16)
        cosine, sine = cos_ref[rows, :], sin_ref[rows, :]
        for head in range(q.shape[1] // HEAD_DIM):
            cols = slice(head * HEAD_DIM, (head + 1) * HEAD_DIM)
            q_ref[rows, cols] = rotate_head(q[:, cols].astype(F32), cosine, sine)


def q_proj(h, wq, cosine, sine):
    rows, width = h.shape
    cols = wq.shape[1]
    tile = 512
    return pl.pallas_call(
        q_kernel,
        grid=(cols // tile,),
        in_specs=[
            pl.BlockSpec((rows, width), lambda i: (0, 0)),
            pl.BlockSpec((width, tile), lambda i: (0, i)),
            pl.BlockSpec((rows, HEAD_DIM), lambda i: (0, 0)),
            pl.BlockSpec((rows, HEAD_DIM), lambda i: (0, 0)),
        ],
        out_specs=pl.BlockSpec((rows, tile), lambda i: (0, i)),
        out_shape=jax.ShapeDtypeStruct((rows, cols), BF16),
        cost_estimate=cost(2 * rows * width * cols, 2 * rows * width + 2 * width * cols),
        name='q_proj',
    )(h, wq, cosine, sine)


def attend_kernel(base, tile, chunk, group, blocks, flags_ref, q_ref, *refs):
    sources = refs[:1 + sum(blocks)]
    o_ref, m_ref, l_ref, acc_ref, s0_ref, s1_ref = refs[1 + sum(blocks):]
    scale2 = (HEAD_DIM ** -0.5) * LOG2E
    step = pl.program_id(1)

    def scores(kv, keys, j, buffer, masked):
        q = q_ref[:, j * HEAD_DIM:(j + 1) * HEAD_DIM]
        top = None
        for start in range(0, keys, chunk):
            size = min(chunk, keys - start)
            s = lax.dot_general(kv[0, start:start + size, :], q, (((1,), (1,)), ((), ())), preferred_element_type=F32)
            if masked and start + size > keys - tile:
                key = lax.broadcasted_iota(jnp.int32, s.shape, 0) + start
                query = lax.broadcasted_iota(jnp.int32, s.shape, 1) + (keys - tile)
                s = jnp.where(key <= query, s, -jnp.inf)
            buffer[start:start + size, :] = s
            part = jnp.max(s.reshape(size // 8, 8, tile), axis=0)
            top = part if top is None else jnp.maximum(top, part)
        return top

    def block(full, keys, first, masked):
        items = [(kv, j) for kv in full for j in range(group)]
        buffers = (s0_ref, s1_ref)
        top8 = scores(items[0][0], keys, items[0][1], buffers[0], masked)
        for n, (kv, j) in enumerate(items):
            top = jnp.max(top8, axis=0, keepdims=True)
            if not first:
                old = m_ref[j]
                top = jnp.maximum(top, old)
            if n + 1 < len(items):
                top8 = scores(items[n + 1][0], keys, items[n + 1][1], buffers[(n + 1) % 2], masked)
            total = part = None
            for start in range(0, keys, chunk):
                size = min(chunk, keys - start)
                e = jnp.exp2((buffers[n % 2][start:start + size, :] - top) * scale2)
                e8 = jnp.sum(e.reshape(size // 8, 8, tile), axis=0)
                vt = jnp.concatenate([kv[1, at:at + HEAD_DIM, :] for at in range(start, start + size, HEAD_DIM)], axis=1)
                product = lax.dot_general(vt, e.astype(BF16), (((1,), (0,)), ((), ())), preferred_element_type=F32)
                total = e8 if total is None else total + e8
                part = product if part is None else part + product
            total = jnp.sum(total, axis=0, keepdims=True)
            if not first:
                factor = jnp.exp2((old - top) * scale2)
                total = total + l_ref[j] * factor
                part = part + acc_ref[j] * factor
            m_ref[j] = top
            l_ref[j] = total
            acc_ref[j] = part

    for n in range(pl.num_programs(1)):

        @pl.when(step == n)
        def _():
            block(sources[:1], base + (n + 1) * tile, True, True)

    start = 1
    for flag, many in enumerate(blocks):
        full = sources[start:start + many]
        start += many

        @pl.when(flags_ref[flag] > 0)
        def _():
            block(full, full[0].shape[1], False, False)

    for j in range(group):
        out = acc_ref[j] / l_ref[j]
        o_ref[:, j * HEAD_DIM:(j + 1) * HEAD_DIM] = out.T.astype(BF16)


def attend(flags, q, base, count, groups, sources, blocks, tile):
    keys = sources[0].shape[2]
    width = q.shape[1] // groups
    group = width // HEAD_DIM
    first = base // tile

    kv_spec = pl.BlockSpec((None, 2, keys, HEAD_DIM), lambda g, i, f: (g, 0, 0, 0))
    grid_spec = pltpu.PrefetchScalarGridSpec(
        num_scalar_prefetch=1,
        grid=(groups, count // tile),
        in_specs=[pl.BlockSpec((tile, width), lambda g, i, f: (first + i, g))] + [kv_spec] * len(sources),
        out_specs=pl.BlockSpec((tile, width), lambda g, i, f: (i, g)),
        scratch_shapes=[
            pltpu.VMEM((group, 1, tile), F32),
            pltpu.VMEM((group, 1, tile), F32),
            pltpu.VMEM((group, HEAD_DIM, tile), F32),
            pltpu.VMEM((keys, tile), F32),
            pltpu.VMEM((keys, tile), F32),
        ],
    )
    return pl.pallas_call(
        functools.partial(attend_kernel, base, tile, 512, group, blocks),
        grid_spec=grid_spec,
        out_shape=jax.ShapeDtypeStruct((count, q.shape[1]), BF16),
        cost_estimate=cost(10 * count * keys * q.shape[1], 4 * len(sources) * keys * groups * HEAD_DIM, 3 * count * keys * groups * group),
        name='attend',
    )(flags, q, *sources)


def gate_up_kernel(h_ref, wg_ref, wu_ref, a_ref):
    gate = jnp.dot(h_ref[...], wg_ref[...], preferred_element_type=F32).astype(BF16).astype(F32)
    up = jnp.dot(h_ref[...], wu_ref[...], preferred_element_type=F32).astype(BF16).astype(F32)
    a_ref[...] = (gate * jax.nn.sigmoid(gate) * up).astype(BF16)


def gate_up(h, wg, wu, first, rows, col, cols):
    width = wg.shape[0]
    tile = 512
    index, start = first // rows, col // tile
    weight_spec = pl.BlockSpec((width, tile), lambda i: (0, start + i))
    return pl.pallas_call(
        gate_up_kernel,
        grid=(cols // tile,),
        in_specs=[pl.BlockSpec((rows, width), lambda i: (index, 0)), weight_spec, weight_spec],
        out_specs=pl.BlockSpec((rows, tile), lambda i: (0, i)),
        out_shape=jax.ShapeDtypeStruct((rows, cols), BF16),
        cost_estimate=cost(4 * rows * width * cols, 2 * rows * (width + cols) + 4 * width * cols),
        name='gate_up',
    )(h, wg, wu)


def down_kernel(acts, attns, streams, *refs):
    a_refs, o_refs = refs[:acts], refs[acts:acts + attns]
    w_refs, wo_ref, out_ref = refs[acts + attns:acts + attns + streams], refs[-2], refs[-1]
    depth = w_refs[0].shape[0]
    rows = out_ref.shape[0] // attns
    a_parts = [a_ref.at[:, start:start + depth] for a_ref in a_refs for start in range(0, a_ref.shape[1], depth)]
    for n, o_ref in enumerate(o_refs):
        place = slice(n * rows, (n + 1) * rows)
        total = jnp.dot(o_ref[...], wo_ref[...], preferred_element_type=F32)
        for a_part, w_ref in zip(a_parts, w_refs):
            total += jnp.dot(a_part[place, :], w_ref[...], preferred_element_type=F32)
        out_ref[place, :] = total.astype(BF16)


def down(acts, attns, wd, wo, rows, col, cols):
    tile = 512
    start = col // tile
    streams = 1
    depth = wd.shape[0] // streams

    def act_spec(array, row):
        return pl.BlockSpec((rows, array.shape[1]), lambda i: (row // rows, 0))

    def stream_spec(n):
        return pl.BlockSpec((depth, tile), lambda i: (n, start + i))

    return pl.pallas_call(
        functools.partial(down_kernel, len(acts), len(attns), streams),
        grid=(cols // tile,),
        in_specs=[act_spec(*pair) for pair in acts]
        + [pl.BlockSpec(o.shape, lambda i: (0, 0)) for o in attns]
        + [stream_spec(n) for n in range(streams)]
        + [pl.BlockSpec((wo.shape[0], tile), lambda i: (0, start + i))],
        out_specs=pl.BlockSpec((rows, tile), lambda i: (0, i)),
        out_shape=jax.ShapeDtypeStruct((rows, cols), BF16),
        cost_estimate=cost(2 * rows * (wd.shape[0] + wo.shape[0]) * cols, 2 * cols * (wd.shape[0] + wo.shape[0])),
        name='down',
    )(*[array for array, _ in acts], *attns, *[wd] * streams, wo)


def add_kernel(x_ref, mine_ref, other_ref, *refs):
    total = mine_ref[...].astype(F32) + other_ref[...].astype(F32)
    refs[-1][...] = (x_ref[...].astype(F32) + total).astype(BF16)


def add_chunk(x, mine, other, out, first, col):
    rows, cols = mine.shape
    tile = 256
    index, start = first // tile, col // cols
    place = pl.BlockSpec((tile, cols), lambda i: (index + i, start))
    chunk = pl.BlockSpec((tile, cols), lambda i: (i, 0))
    args, specs, alias = [x, mine, other], [place, chunk, chunk], {}
    if out is not None:
        args, specs, alias = args + [out], specs + [pl.BlockSpec(memory_space=pl.ANY)], {3: 0}
    return pl.pallas_call(
        add_kernel,
        grid=(rows // tile,),
        in_specs=specs,
        out_specs=place,
        out_shape=jax.ShapeDtypeStruct(x.shape, BF16),
        input_output_aliases=alias,
        cost_estimate=cost(3 * rows * cols, 8 * rows * cols),
        name='add',
    )(*args)


SCHEDULE = (
    ('mlp', 0, 512, 0, 4096),
    ('own', 0, 512, 512),
    ('down', 0, 512, 0, 3072),
    ('mlp', 512, 512, 0, 4096),
    ('own', 512, 512, 512),
    ('down', 512, 512, 1024, 512),
    ('down', 512, 512, 0, 1024),
    ('down', 512, 512, 1536, 1536),
)


def solution(mesh):
    if mesh.shape['cp'] != 4 or mesh.shape['tp'] != 2:
        raise ValueError('mesh')

    def local_layer(hidden, positions, ln_gain, w_q, w_k, w_v, w_o, w_gate, w_up, w_down):
        me = lax.axis_index('cp')
        cosine, sine = rotary_tables(positions)
        normed, kv_own, k_own, v_own = norm_kv(hidden, ln_gain, w_k, w_v, cosine, sine)
        groups = kv_own.shape[0]
        send = functools.partial(lax.ppermute, axis_name='cp')
        kv_b = send(kv_own, perm=[(0, 2), (1, 3)])
        kv_a = send(kv_own, perm=[(0, 1), (2, 3)])
        kv_c = send(kv_b, perm=[(2, 3), (3, 2)])
        cache_shape = (k_own.shape[0], groups, HEAD_DIM)
        k_cache, v_cache = k_own.reshape(cache_shape), v_own.reshape(cache_shape)
        flags = jnp.stack([me % 2, me // 2]).astype(jnp.int32)
        q_rot = q_proj(normed, w_q, cosine, sine)
        last = q_rot
        acts, attns, pieces = [], [], []
        for kind, first, rows, *place in SCHEDULE:
            if kind == 'mlp':
                normed, last = lax.optimization_barrier((normed, last))
                last = gate_up(normed, w_gate, w_up, first, rows, *place)
                acts.append((first, rows, last))
            if kind == 'own':
                q_rot, last = lax.optimization_barrier((q_rot, last))
                sources = (kv_own, kv_a, kv_b, kv_c)
                last = attend(flags, q_rot, first, rows, groups, sources, (1, 2), *place)
                attns.append((first, last))
            if kind == 'down':
                col, cols = place
                act = [(array, first - start) for start, many, array in acts if start <= first < start + many]
                attn = [array for start, array in attns if first <= start < first + rows]
                attn, last = lax.optimization_barrier((attn, last))
                last = down(act, attn, w_down, w_o, rows, col, cols)
                other = lax.ppermute(last, 'tp', [(0, 1), (1, 0)])
                pieces.append((last, other, first, col))
        hidden_out = None
        for part, other, first, col in pieces:
            hidden_out = add_chunk(hidden, part, other, hidden_out, first, col)
        return hidden_out, k_cache, v_cache

    row_spec = P(('dp', 'cp'), None)
    col_spec = P(None, 'tp')
    cache_spec = P(('dp', 'cp'), 'tp', None)
    in_specs = (row_spec, P(('dp', 'cp')), P(None), col_spec, col_spec, col_spec, P('tp', None), col_spec, col_spec, P('tp', None))
    return jax.shard_map(local_layer, mesh=mesh, in_specs=in_specs, out_specs=(row_spec, cache_spec, cache_spec), check_vma=False)
```

```python
import functools

import jax
import jax.numpy as jnp
from jax import lax
from jax.experimental import pallas as pl
from jax.experimental.pallas import tpu as pltpu
from jax.sharding import PartitionSpec as P


HEAD_DIM = 128
ROPE_BASE = 4000000
LN_EPS = 1e-5
LOG2E = 1.4426950408889634
BF16 = jnp.bfloat16
F32 = jnp.float32


def cost(flops, bytes_accessed, transcendentals=0):
    return pl.CostEstimate(flops=int(flops), bytes_accessed=int(bytes_accessed), transcendentals=int(transcendentals))


def rotary_tables(positions):
    lane = jnp.arange(HEAD_DIM)
    exponent = ((lane // 2) * 2).astype(F32) / HEAD_DIM
    inv_freq = 1.0 / (ROPE_BASE ** exponent)
    angles = positions.astype(F32)[:, None] * inv_freq[None, :]
    sign = jnp.where(lane % 2 == 0, -1.0, 1.0).astype(F32)
    return jnp.cos(angles), jnp.sin(angles) * sign[None, :]


def rotate_head(head, cosine, sine):
    even = lax.broadcasted_iota(jnp.int32, head.shape, 1) % 2 == 0
    other = jnp.where(even, pltpu.roll(head, HEAD_DIM - 1, 1), pltpu.roll(head, 1, 1))
    return (head * cosine + other * sine).astype(BF16)


def norm_kv_kernel(x_ref, gain_ref, wk_hbm, wv_hbm, cos_ref, sin_ref, h_ref, kv_ref, k_ref, v_ref, wk_ref, wv_ref, sems):
    copies = [pltpu.make_async_copy(wk_hbm, wk_ref, sems.at[0]), pltpu.make_async_copy(wv_hbm, wv_ref, sems.at[1])]

    @pl.when(pl.program_id(0) == 0)
    def _():
        for copy in copies:
            copy.start()

    x = x_ref[...].astype(F32)
    width = x.shape[1]
    mean = jnp.sum(x, axis=1, keepdims=True) * (1.0 / width)
    centered = x - mean
    var = jnp.sum(centered * centered, axis=1, keepdims=True) * (1.0 / width)
    h_ref[...] = (centered * lax.rsqrt(var + LN_EPS) * gain_ref[...].astype(F32)[None, :]).astype(BF16)

    @pl.when(pl.program_id(0) == 0)
    def _():
        for copy in copies:
            copy.wait()

    k = jnp.dot(h_ref[...], wk_ref[...], preferred_element_type=F32).astype(BF16)
    v = jnp.dot(h_ref[...], wv_ref[...], preferred_element_type=F32).astype(BF16)
    v_ref[...] = v
    cosine, sine = cos_ref[...], sin_ref[...]
    for head in range(k.shape[1] // HEAD_DIM):
        cols = slice(head * HEAD_DIM, (head + 1) * HEAD_DIM)
        rotated = rotate_head(k[:, cols].astype(F32), cosine, sine)
        k_ref[:, cols] = rotated
        kv_ref[head, 0] = rotated
        for start in range(0, k.shape[0], HEAD_DIM):
            kv_ref[head, 1, start:start + HEAD_DIM, :] = v[start:start + HEAD_DIM, cols].T


def norm_kv(x, gain, wk, wv, cosine, sine):
    rows, width = x.shape
    kv = wk.shape[1]
    groups = kv // HEAD_DIM
    tile = 256
    return pl.pallas_call(
        norm_kv_kernel,
        grid=(rows // tile,),
        in_specs=[
            pl.BlockSpec((tile, width), lambda i: (i, 0)),
            pl.BlockSpec((width,), lambda i: (0,)),
            pl.BlockSpec(memory_space=pl.ANY),
            pl.BlockSpec(memory_space=pl.ANY),
            pl.BlockSpec((tile, HEAD_DIM), lambda i: (i, 0)),
            pl.BlockSpec((tile, HEAD_DIM), lambda i: (i, 0)),
        ],
        out_specs=[
            pl.BlockSpec((tile, width), lambda i: (i, 0)),
            pl.BlockSpec((groups, 2, tile, HEAD_DIM), lambda i: (0, 0, i, 0)),
            pl.BlockSpec((tile, kv), lambda i: (i, 0)),
            pl.BlockSpec((tile, kv), lambda i: (i, 0)),
        ],
        out_shape=[
            jax.ShapeDtypeStruct((rows, width), BF16),
            jax.ShapeDtypeStruct((groups, 2, rows, HEAD_DIM), BF16),
            jax.ShapeDtypeStruct((rows, kv), BF16),
            jax.ShapeDtypeStruct((rows, kv), BF16),
        ],
        scratch_shapes=[pltpu.VMEM((width, kv), BF16), pltpu.VMEM((width, kv), BF16), pltpu.SemaphoreType.DMA((2,))],
        cost_estimate=cost(4 * rows * width * kv, 4 * rows * width + 4 * width * kv),
        name='norm_kv',
    )(x, gain, wk, wv, cosine, sine)


def q_kernel(h_ref, w_ref, cos_ref, sin_ref, q_ref):
    q = jnp.dot(h_ref[...], w_ref[...], preferred_element_type=F32).astype(BF16)
    cosine, sine = cos_ref[...], sin_ref[...]
    for head in range(q.shape[1] // HEAD_DIM):
        cols = slice(head * HEAD_DIM, (head + 1) * HEAD_DIM)
        q_ref[:, cols] = rotate_head(q[:, cols].astype(F32), cosine, sine)


def q_proj(h, wq, cosine, sine):
    rows, width = h.shape
    cols = wq.shape[1]
    tile, half = 512, 512
    return pl.pallas_call(
        q_kernel,
        grid=(rows // half, cols // tile),
        in_specs=[
            pl.BlockSpec((half, width), lambda r, i: (r, 0)),
            pl.BlockSpec((width, tile), lambda r, i: (0, i)),
            pl.BlockSpec((half, HEAD_DIM), lambda r, i: (r, 0)),
            pl.BlockSpec((half, HEAD_DIM), lambda r, i: (r, 0)),
        ],
        out_specs=pl.BlockSpec((half, tile), lambda r, i: (r, i)),
        out_shape=jax.ShapeDtypeStruct((rows, cols), BF16),
        cost_estimate=cost(2 * rows * width * cols, 2 * rows * width + 2 * width * cols),
        name='q_proj',
    )(h, wq, cosine, sine)


def attend_kernel(base, tile, chunk, group, blocks, flags_ref, q_ref, *refs):
    sources = refs[:1 + sum(blocks)]
    o_ref, m_ref, l_ref, acc_ref, s0_ref, s1_ref = refs[1 + sum(blocks):]
    scale2 = (HEAD_DIM ** -0.5) * LOG2E
    step = pl.program_id(1)

    def scores(kv, keys, j, buffer, masked):
        q = q_ref[:, j * HEAD_DIM:(j + 1) * HEAD_DIM]
        top = None
        for start in range(0, keys, chunk):
            size = min(chunk, keys - start)
            s = lax.dot_general(kv[0, start:start + size, :], q, (((1,), (1,)), ((), ())), preferred_element_type=F32)
            if masked and start + size > keys - tile:
                key = lax.broadcasted_iota(jnp.int32, s.shape, 0) + start
                query = lax.broadcasted_iota(jnp.int32, s.shape, 1) + (keys - tile)
                s = jnp.where(key <= query, s, -jnp.inf)
            buffer[start:start + size, :] = s
            part = jnp.max(s.reshape(size // 8, 8, tile), axis=0)
            top = part if top is None else jnp.maximum(top, part)
        return top

    def block(full, keys, first, masked):
        items = [(kv, j) for kv in full for j in range(group)]
        buffers = (s0_ref, s1_ref)
        top8 = scores(items[0][0], keys, items[0][1], buffers[0], masked)
        for n, (kv, j) in enumerate(items):
            top = jnp.max(top8, axis=0, keepdims=True)
            if not first:
                old = m_ref[j]
                top = jnp.maximum(top, old)
            if n + 1 < len(items):
                top8 = scores(items[n + 1][0], keys, items[n + 1][1], buffers[(n + 1) % 2], masked)
            total = part = None
            for start in range(0, keys, chunk):
                size = min(chunk, keys - start)
                e = jnp.exp2((buffers[n % 2][start:start + size, :] - top) * scale2)
                e8 = jnp.sum(e.reshape(size // 8, 8, tile), axis=0)
                vt = jnp.concatenate([kv[1, at:at + HEAD_DIM, :] for at in range(start, start + size, HEAD_DIM)], axis=1)
                product = lax.dot_general(vt, e.astype(BF16), (((1,), (0,)), ((), ())), preferred_element_type=F32)
                total = e8 if total is None else total + e8
                part = product if part is None else part + product
            total = jnp.sum(total, axis=0, keepdims=True)
            if not first:
                factor = jnp.exp2((old - top) * scale2)
                total = total + l_ref[j] * factor
                part = part + acc_ref[j] * factor
            m_ref[j] = top
            l_ref[j] = total
            acc_ref[j] = part

    for n in range(pl.num_programs(1)):

        @pl.when(step == n)
        def _():
            block(sources[:1], base + (n + 1) * tile, True, True)

    start = 1
    for flag, many in enumerate(blocks):
        full = sources[start:start + many]
        start += many

        @pl.when(flags_ref[flag] > 0)
        def _():
            block(full, full[0].shape[1], False, False)

    for j in range(group):
        out = acc_ref[j] / l_ref[j]
        o_ref[:, j * HEAD_DIM:(j + 1) * HEAD_DIM] = out.T.astype(BF16)


def attend(flags, q, base, count, groups, sources, blocks, tile):
    keys = sources[0].shape[2]
    width = q.shape[1] // groups
    group = width // HEAD_DIM
    first = base // tile

    kv_spec = pl.BlockSpec((None, 2, keys, HEAD_DIM), lambda g, i, f: (g, 0, 0, 0))
    grid_spec = pltpu.PrefetchScalarGridSpec(
        num_scalar_prefetch=1,
        grid=(groups, count // tile),
        in_specs=[pl.BlockSpec((tile, width), lambda g, i, f: (first + i, g))] + [kv_spec] * len(sources),
        out_specs=pl.BlockSpec((tile, width), lambda g, i, f: (i, g)),
        scratch_shapes=[
            pltpu.VMEM((group, 1, tile), F32),
            pltpu.VMEM((group, 1, tile), F32),
            pltpu.VMEM((group, HEAD_DIM, tile), F32),
            pltpu.VMEM((keys, tile), F32),
            pltpu.VMEM((keys, tile), F32),
        ],
    )
    return pl.pallas_call(
        functools.partial(attend_kernel, base, tile, 512, group, blocks),
        grid_spec=grid_spec,
        out_shape=jax.ShapeDtypeStruct((count, q.shape[1]), BF16),
        cost_estimate=cost(10 * count * keys * q.shape[1], 4 * len(sources) * keys * groups * HEAD_DIM, 3 * count * keys * groups * group),
        name='attend',
    )(flags, q, *sources)


def gate_up_kernel(h_ref, wg_ref, wu_ref, a_ref):
    gate = jnp.dot(h_ref[...], wg_ref[...], preferred_element_type=F32).astype(BF16).astype(F32)
    up = jnp.dot(h_ref[...], wu_ref[...], preferred_element_type=F32).astype(BF16).astype(F32)
    a_ref[...] = (gate * jax.nn.sigmoid(gate) * up).astype(BF16)


def gate_up(h, wg, wu, first, rows, col, cols):
    width = wg.shape[0]
    tile = 256 if first == 0 else 512
    index, start = first // rows, col // tile
    weight_spec = pl.BlockSpec((width, tile), lambda i: (0, start + i))
    return pl.pallas_call(
        gate_up_kernel,
        grid=(cols // tile,),
        in_specs=[pl.BlockSpec((rows, width), lambda i: (index, 0)), weight_spec, weight_spec],
        out_specs=pl.BlockSpec((rows, tile), lambda i: (0, i)),
        out_shape=jax.ShapeDtypeStruct((rows, cols), BF16),
        cost_estimate=cost(4 * rows * width * cols, 2 * rows * (width + cols) + 4 * width * cols),
        name='gate_up',
    )(h, wg, wu)


def down_kernel(acts, attns, streams, *refs):
    a_refs, o_refs = refs[:acts], refs[acts:acts + attns]
    w_refs, wo_ref, out_ref = refs[acts + attns:acts + attns + streams], refs[-2], refs[-1]
    depth = w_refs[0].shape[0]
    rows = out_ref.shape[0] // attns
    a_parts = [a_ref.at[:, start:start + depth] for a_ref in a_refs for start in range(0, a_ref.shape[1], depth)]
    for n, o_ref in enumerate(o_refs):
        place = slice(n * rows, (n + 1) * rows)
        total = jnp.dot(o_ref[...], wo_ref[...], preferred_element_type=F32)
        for a_part, w_ref in zip(a_parts, w_refs):
            total += jnp.dot(a_part[place, :], w_ref[...], preferred_element_type=F32)
        out_ref[place, :] = total.astype(BF16)


def down(acts, attns, wd, wo, rows, col, cols):
    tile = 512
    start = col // tile
    streams = 1
    depth = wd.shape[0] // streams

    def act_spec(array, row):
        return pl.BlockSpec((rows, array.shape[1]), lambda i: (row // rows, 0))

    def stream_spec(n):
        return pl.BlockSpec((depth, tile), lambda i: (n, start + i))

    return pl.pallas_call(
        functools.partial(down_kernel, len(acts), len(attns), streams),
        grid=(cols // tile,),
        in_specs=[act_spec(*pair) for pair in acts]
        + [pl.BlockSpec(o.shape, lambda i: (0, 0)) for o in attns]
        + [stream_spec(n) for n in range(streams)]
        + [pl.BlockSpec((wo.shape[0], tile), lambda i: (0, start + i))],
        out_specs=pl.BlockSpec((rows, tile), lambda i: (0, i)),
        out_shape=jax.ShapeDtypeStruct((rows, cols), BF16),
        cost_estimate=cost(2 * rows * (wd.shape[0] + wo.shape[0]) * cols, 2 * cols * (wd.shape[0] + wo.shape[0])),
        name='down',
    )(*[array for array, _ in acts], *attns, *[wd] * streams, wo)


def add_kernel(x_ref, mine_ref, other_ref, *refs):
    total = mine_ref[...].astype(F32) + other_ref[...].astype(F32)
    refs[-1][...] = (x_ref[...].astype(F32) + total).astype(BF16)


def add_chunk(x, mine, other, out, first, col):
    rows, cols = mine.shape
    tile = 256
    index, start = first // tile, col // cols
    place = pl.BlockSpec((tile, cols), lambda i: (index + i, start))
    chunk = pl.BlockSpec((tile, cols), lambda i: (i, 0))
    args, specs, alias = [x, mine, other], [place, chunk, chunk], {}
    if out is not None:
        args, specs, alias = args + [out], specs + [pl.BlockSpec(memory_space=pl.ANY)], {3: 0}
    return pl.pallas_call(
        add_kernel,
        grid=(rows // tile,),
        in_specs=specs,
        out_specs=place,
        out_shape=jax.ShapeDtypeStruct(x.shape, BF16),
        input_output_aliases=alias,
        cost_estimate=cost(3 * rows * cols, 8 * rows * cols),
        name='add',
    )(*args)


SCHEDULE = (
    ('mlp', 0, 512, 0, 4096),
    ('own', 0, 512, 512),
    ('down', 0, 512, 0, 3072),
    ('mlp', 512, 512, 0, 4096),
    ('own', 512, 512, 512),
    ('down', 512, 512, 0, 1024),
    ('down', 512, 512, 1536, 1536),
    ('down', 512, 512, 1024, 512),
)


def solution(mesh):
    if mesh.shape['cp'] != 4 or mesh.shape['tp'] != 2:
        raise ValueError('mesh')

    def local_layer(hidden, positions, ln_gain, w_q, w_k, w_v, w_o, w_gate, w_up, w_down):
        me = lax.axis_index('cp')
        cosine, sine = rotary_tables(positions)
        normed, kv_own, k_own, v_own = norm_kv(hidden, ln_gain, w_k, w_v, cosine, sine)
        groups = kv_own.shape[0]
        send = functools.partial(lax.ppermute, axis_name='cp')
        kv_b = send(kv_own, perm=[(0, 2), (1, 3)])
        kv_a = send(kv_own, perm=[(0, 1), (2, 3)])
        kv_c = send(kv_b, perm=[(2, 3), (3, 2)])
        cache_shape = (k_own.shape[0], groups, HEAD_DIM)
        k_cache, v_cache = k_own.reshape(cache_shape), v_own.reshape(cache_shape)
        flags = jnp.stack([me % 2, me // 2]).astype(jnp.int32)
        q_rot = q_proj(normed, w_q, cosine, sine)
        last = q_rot
        acts, attns, pieces = [], [], []
        for kind, first, rows, *place in SCHEDULE:
            if kind == 'mlp':
                normed, last = lax.optimization_barrier((normed, last))
                last = gate_up(normed, w_gate, w_up, first, rows, *place)
                acts.append((first, rows, last))
            if kind == 'own':
                q_rot, last = lax.optimization_barrier((q_rot, last))
                sources = (kv_own, kv_a, kv_b, kv_c)
                last = attend(flags, q_rot, first, rows, groups, sources, (1, 2), *place)
                attns.append((first, last))
            if kind == 'down':
                col, cols = place
                act = [(array, first - start) for start, many, array in acts if start <= first < start + many]
                attn = [array for start, array in attns if first <= start < first + rows]
                attn, last = lax.optimization_barrier((attn, last))
                last = down(act, attn, w_down, w_o, rows, col, cols)
                other = lax.ppermute(last, 'tp', [(0, 1), (1, 0)])
                pieces.append((last, other, first, col))
        hidden_out = None
        for part, other, first, col in pieces:
            hidden_out = add_chunk(hidden, part, other, hidden_out, first, col)
        return hidden_out, k_cache, v_cache

    row_spec = P(('dp', 'cp'), None)
    col_spec = P(None, 'tp')
    cache_spec = P(('dp', 'cp'), 'tp', None)
    in_specs = (row_spec, P(('dp', 'cp')), P(None), col_spec, col_spec, col_spec, P('tp', None), col_spec, col_spec, P('tp', None))
    return jax.shard_map(local_layer, mesh=mesh, in_specs=in_specs, out_specs=(row_spec, cache_spec, cache_spec), check_vma=False)
```

```python
import functools

import jax
import jax.numpy as jnp
from jax import lax
from jax.experimental import pallas as pl
from jax.experimental.pallas import tpu as pltpu
from jax.sharding import PartitionSpec as P


HEAD_DIM = 128
ROPE_BASE = 4000000
LN_EPS = 1e-5
LOG2E = 1.4426950408889634
BF16 = jnp.bfloat16
F32 = jnp.float32


def cost(flops, bytes_accessed, transcendentals=0):
    return pl.CostEstimate(flops=int(flops), bytes_accessed=int(bytes_accessed), transcendentals=int(transcendentals))


def rotary_tables(positions):
    lane = jnp.arange(HEAD_DIM)
    exponent = ((lane // 2) * 2).astype(F32) / HEAD_DIM
    inv_freq = 1.0 / (ROPE_BASE ** exponent)
    angles = positions.astype(F32)[:, None] * inv_freq[None, :]
    sign = jnp.where(lane % 2 == 0, -1.0, 1.0).astype(F32)
    return jnp.cos(angles), jnp.sin(angles) * sign[None, :]


def rotate_head(head, cosine, sine):
    even = lax.broadcasted_iota(jnp.int32, head.shape, 1) % 2 == 0
    other = jnp.where(even, pltpu.roll(head, HEAD_DIM - 1, 1), pltpu.roll(head, 1, 1))
    return (head * cosine + other * sine).astype(BF16)


def norm_kv_kernel(x_ref, gain_ref, wk_ref, wv_ref, cos_ref, sin_ref, h_ref, kv_ref, k_ref, v_ref):
    x = x_ref[...].astype(F32)
    width = x.shape[1]
    mean = jnp.sum(x, axis=1, keepdims=True) * (1.0 / width)
    centered = x - mean
    var = jnp.sum(centered * centered, axis=1, keepdims=True) * (1.0 / width)
    h_ref[...] = (centered * lax.rsqrt(var + LN_EPS) * gain_ref[...].astype(F32)[None, :]).astype(BF16)
    k = jnp.dot(h_ref[...], wk_ref[...], preferred_element_type=F32).astype(BF16)
    v = jnp.dot(h_ref[...], wv_ref[...], preferred_element_type=F32).astype(BF16)
    v_ref[...] = v
    cosine, sine = cos_ref[...], sin_ref[...]
    for head in range(k.shape[1] // HEAD_DIM):
        cols = slice(head * HEAD_DIM, (head + 1) * HEAD_DIM)
        rotated = rotate_head(k[:, cols].astype(F32), cosine, sine)
        k_ref[:, cols] = rotated
        kv_ref[head, 0] = rotated
        for start in range(0, k.shape[0], HEAD_DIM):
            kv_ref[head, 1, start:start + HEAD_DIM, :] = v[start:start + HEAD_DIM, cols].T


def norm_kv(x, gain, wk, wv, cosine, sine):
    rows, width = x.shape
    kv = wk.shape[1]
    groups = kv // HEAD_DIM
    tile = 256
    return pl.pallas_call(
        norm_kv_kernel,
        grid=(rows // tile,),
        in_specs=[
            pl.BlockSpec((tile, width), lambda i: (i, 0)),
            pl.BlockSpec((width,), lambda i: (0,)),
            pl.BlockSpec((width, kv), lambda i: (0, 0)),
            pl.BlockSpec((width, kv), lambda i: (0, 0)),
            pl.BlockSpec((tile, HEAD_DIM), lambda i: (i, 0)),
            pl.BlockSpec((tile, HEAD_DIM), lambda i: (i, 0)),
        ],
        out_specs=[
            pl.BlockSpec((tile, width), lambda i: (i, 0)),
            pl.BlockSpec((groups, 2, tile, HEAD_DIM), lambda i: (0, 0, i, 0)),
            pl.BlockSpec((tile, kv), lambda i: (i, 0)),
            pl.BlockSpec((tile, kv), lambda i: (i, 0)),
        ],
        out_shape=[
            jax.ShapeDtypeStruct((rows, width), BF16),
            jax.ShapeDtypeStruct((groups, 2, rows, HEAD_DIM), BF16),
            jax.ShapeDtypeStruct((rows, kv), BF16),
            jax.ShapeDtypeStruct((rows, kv), BF16),
        ],
        cost_estimate=cost(4 * rows * width * kv, 4 * rows * width + 4 * width * kv),
        name='norm_kv',
    )(x, gain, wk, wv, cosine, sine)


def q_kernel(h_ref, w_ref, cos_ref, sin_ref, q_ref):
    for start in range(0, h_ref.shape[0], 512):
        rows = slice(start, start + 512)
        q = jnp.dot(h_ref[rows, :], w_ref[...], preferred_element_type=F32).astype(BF16)
        cosine, sine = cos_ref[rows, :], sin_ref[rows, :]
        for head in range(q.shape[1] // HEAD_DIM):
            cols = slice(head * HEAD_DIM, (head + 1) * HEAD_DIM)
            q_ref[rows, cols] = rotate_head(q[:, cols].astype(F32), cosine, sine)


def q_proj(h, wq, cosine, sine):
    rows, width = h.shape
    cols = wq.shape[1]
    tile = 512
    return pl.pallas_call(
        q_kernel,
        grid=(cols // tile,),
        in_specs=[
            pl.BlockSpec((rows, width), lambda i: (0, 0)),
            pl.BlockSpec((width, tile), lambda i: (0, i)),
            pl.BlockSpec((rows, HEAD_DIM), lambda i: (0, 0)),
            pl.BlockSpec((rows, HEAD_DIM), lambda i: (0, 0)),
        ],
        out_specs=pl.BlockSpec((rows, tile), lambda i: (0, i)),
        out_shape=jax.ShapeDtypeStruct((rows, cols), BF16),
        cost_estimate=cost(2 * rows * width * cols, 2 * rows * width + 2 * width * cols),
        name='q_proj',
    )(h, wq, cosine, sine)


def attend_kernel(base, tile, chunk, group, blocks, flags_ref, q_ref, *refs):
    sources = refs[:1 + sum(blocks)]
    o_ref, m_ref, l_ref, acc_ref, s0_ref, s1_ref = refs[1 + sum(blocks):]
    scale2 = (HEAD_DIM ** -0.5) * LOG2E
    step = pl.program_id(1)

    def scores(kv, keys, j, buffer, masked):
        q = q_ref[:, j * HEAD_DIM:(j + 1) * HEAD_DIM]
        top = None
        for start in range(0, keys, chunk):
            size = min(chunk, keys - start)
            s = lax.dot_general(kv[0, start:start + size, :], q, (((1,), (1,)), ((), ())), preferred_element_type=F32)
            if masked and start + size > keys - tile:
                key = lax.broadcasted_iota(jnp.int32, s.shape, 0) + start
                query = lax.broadcasted_iota(jnp.int32, s.shape, 1) + (keys - tile)
                s = jnp.where(key <= query, s, -jnp.inf)
            buffer[start:start + size, :] = s
            part = jnp.max(s.reshape(size // 8, 8, tile), axis=0)
            top = part if top is None else jnp.maximum(top, part)
        return top

    def block(full, keys, first, masked):
        items = [(kv, j) for kv in full for j in range(group)]
        buffers = (s0_ref, s1_ref)
        top8 = scores(items[0][0], keys, items[0][1], buffers[0], masked)
        for n, (kv, j) in enumerate(items):
            top = jnp.max(top8, axis=0, keepdims=True)
            if not first:
                old = m_ref[j]
                top = jnp.maximum(top, old)
            if n + 1 < len(items):
                top8 = scores(items[n + 1][0], keys, items[n + 1][1], buffers[(n + 1) % 2], masked)
            total = part = None
            for start in range(0, keys, chunk):
                size = min(chunk, keys - start)
                e = jnp.exp2((buffers[n % 2][start:start + size, :] - top) * scale2)
                e8 = jnp.sum(e.reshape(size // 8, 8, tile), axis=0)
                vt = jnp.concatenate([kv[1, at:at + HEAD_DIM, :] for at in range(start, start + size, HEAD_DIM)], axis=1)
                product = lax.dot_general(vt, e.astype(BF16), (((1,), (0,)), ((), ())), preferred_element_type=F32)
                total = e8 if total is None else total + e8
                part = product if part is None else part + product
            total = jnp.sum(total, axis=0, keepdims=True)
            if not first:
                factor = jnp.exp2((old - top) * scale2)
                total = total + l_ref[j] * factor
                part = part + acc_ref[j] * factor
            m_ref[j] = top
            l_ref[j] = total
            acc_ref[j] = part

    for n in range(pl.num_programs(1)):

        @pl.when(step == n)
        def _():
            block(sources[:1], base + (n + 1) * tile, True, True)

    start = 1
    for flag, many in enumerate(blocks):
        full = sources[start:start + many]
        start += many

        @pl.when(flags_ref[flag] > 0)
        def _():
            block(full, full[0].shape[1], False, False)

    for j in range(group):
        out = acc_ref[j] / l_ref[j]
        o_ref[:, j * HEAD_DIM:(j + 1) * HEAD_DIM] = out.T.astype(BF16)


def attend(flags, q, base, count, groups, sources, blocks, tile):
    keys = sources[0].shape[2]
    width = q.shape[1] // groups
    group = width // HEAD_DIM
    first = base // tile

    kv_spec = pl.BlockSpec((None, 2, keys, HEAD_DIM), lambda g, i, f: (g, 0, 0, 0))
    grid_spec = pltpu.PrefetchScalarGridSpec(
        num_scalar_prefetch=1,
        grid=(groups, count // tile),
        in_specs=[pl.BlockSpec((tile, width), lambda g, i, f: (first + i, g))] + [kv_spec] * len(sources),
        out_specs=pl.BlockSpec((tile, width), lambda g, i, f: (i, g)),
        scratch_shapes=[
            pltpu.VMEM((group, 1, tile), F32),
            pltpu.VMEM((group, 1, tile), F32),
            pltpu.VMEM((group, HEAD_DIM, tile), F32),
            pltpu.VMEM((keys, tile), F32),
            pltpu.VMEM((keys, tile), F32),
        ],
    )
    return pl.pallas_call(
        functools.partial(attend_kernel, base, tile, 512, group, blocks),
        grid_spec=grid_spec,
        out_shape=jax.ShapeDtypeStruct((count, q.shape[1]), BF16),
        cost_estimate=cost(10 * count * keys * q.shape[1], 4 * len(sources) * keys * groups * HEAD_DIM, 3 * count * keys * groups * group),
        name='attend',
    )(flags, q, *sources)


def gate_up_kernel(h_ref, wg_ref, wu_ref, a_ref):
    gate = jnp.dot(h_ref[...], wg_ref[...], preferred_element_type=F32).astype(BF16).astype(F32)
    up = jnp.dot(h_ref[...], wu_ref[...], preferred_element_type=F32).astype(BF16).astype(F32)
    a_ref[...] = (gate * jax.nn.sigmoid(gate) * up).astype(BF16)


def gate_up(h, wg, wu, first, rows, col, cols):
    width = wg.shape[0]
    tile = 512
    index, start = first // rows, col // tile
    weight_spec = pl.BlockSpec((width, tile), lambda i: (0, start + i))
    return pl.pallas_call(
        gate_up_kernel,
        grid=(cols // tile,),
        in_specs=[pl.BlockSpec((rows, width), lambda i: (index, 0)), weight_spec, weight_spec],
        out_specs=pl.BlockSpec((rows, tile), lambda i: (0, i)),
        out_shape=jax.ShapeDtypeStruct((rows, cols), BF16),
        cost_estimate=cost(4 * rows * width * cols, 2 * rows * (width + cols) + 4 * width * cols),
        name='gate_up',
    )(h, wg, wu)


def down_kernel(acts, attns, streams, *refs):
    a_refs, o_refs = refs[:acts], refs[acts:acts + attns]
    w_refs, wo_ref, out_ref = refs[acts + attns:acts + attns + streams], refs[-2], refs[-1]
    depth = w_refs[0].shape[0]
    rows = out_ref.shape[0] // attns
    a_parts = [a_ref.at[:, start:start + depth] for a_ref in a_refs for start in range(0, a_ref.shape[1], depth)]
    for n, o_ref in enumerate(o_refs):
        place = slice(n * rows, (n + 1) * rows)
        total = jnp.dot(o_ref[...], wo_ref[...], preferred_element_type=F32)
        for a_part, w_ref in zip(a_parts, w_refs):
            total += jnp.dot(a_part[place, :], w_ref[...], preferred_element_type=F32)
        out_ref[place, :] = total.astype(BF16)


def down(acts, attns, wd, wo, rows, col, cols):
    tile = 512
    start = col // tile
    streams = 1
    depth = wd.shape[0] // streams

    def act_spec(array, row):
        return pl.BlockSpec((rows, array.shape[1]), lambda i: (row // rows, 0))

    def stream_spec(n):
        return pl.BlockSpec((depth, tile), lambda i: (n, start + i))

    return pl.pallas_call(
        functools.partial(down_kernel, len(acts), len(attns), streams),
        grid=(cols // tile,),
        in_specs=[act_spec(*pair) for pair in acts]
        + [pl.BlockSpec(o.shape, lambda i: (0, 0)) for o in attns]
        + [stream_spec(n) for n in range(streams)]
        + [pl.BlockSpec((wo.shape[0], tile), lambda i: (0, start + i))],
        out_specs=pl.BlockSpec((rows, tile), lambda i: (0, i)),
        out_shape=jax.ShapeDtypeStruct((rows, cols), BF16),
        cost_estimate=cost(2 * rows * (wd.shape[0] + wo.shape[0]) * cols, 2 * cols * (wd.shape[0] + wo.shape[0])),
        name='down',
    )(*[array for array, _ in acts], *attns, *[wd] * streams, wo)


def add_kernel(x_ref, mine_ref, other_ref, *refs):
    total = mine_ref[...].astype(F32) + other_ref[...].astype(F32)
    refs[-1][...] = (x_ref[...].astype(F32) + total).astype(BF16)


def add_chunk(x, mine, other, out, first, col):
    rows, cols = mine.shape
    tile = 256
    index, start = first // tile, col // cols
    place = pl.BlockSpec((tile, cols), lambda i: (index + i, start))
    chunk = pl.BlockSpec((tile, cols), lambda i: (i, 0))
    args, specs, alias = [x, mine, other], [place, chunk, chunk], {}
    if out is not None:
        args, specs, alias = args + [out], specs + [pl.BlockSpec(memory_space=pl.ANY)], {3: 0}
    return pl.pallas_call(
        add_kernel,
        grid=(rows // tile,),
        in_specs=specs,
        out_specs=place,
        out_shape=jax.ShapeDtypeStruct(x.shape, BF16),
        input_output_aliases=alias,
        cost_estimate=cost(3 * rows * cols, 8 * rows * cols),
        name='add',
    )(*args)


SCHEDULE = (
    ('mlp', 0, 512, 0, 4096),
    ('own', 0, 512, 512),
    ('down', 0, 512, 2560, 512),
    ('down', 0, 512, 0, 2560),
    ('mlp', 512, 512, 0, 4096),
    ('own', 512, 256, 256),
    ('down', 512, 256, 0, 3072),
    ('own', 768, 256, 256),
    ('down', 768, 256, 0, 1536),
    ('down', 768, 256, 1536, 1536),
)


def solution(mesh):
    if mesh.shape['cp'] != 4 or mesh.shape['tp'] != 2:
        raise ValueError('mesh')

    def local_layer(hidden, positions, ln_gain, w_q, w_k, w_v, w_o, w_gate, w_up, w_down):
        me = lax.axis_index('cp')
        cosine, sine = rotary_tables(positions)
        normed, kv_own, k_own, v_own = norm_kv(hidden, ln_gain, w_k, w_v, cosine, sine)
        groups = kv_own.shape[0]
        send = functools.partial(lax.ppermute, axis_name='cp')
        kv_b = send(kv_own, perm=[(0, 2), (1, 3)])
        kv_a = send(kv_own, perm=[(0, 1), (2, 3)])
        kv_c = send(kv_b, perm=[(2, 3), (3, 2)])
        cache_shape = (k_own.shape[0], groups, HEAD_DIM)
        k_cache, v_cache = k_own.reshape(cache_shape), v_own.reshape(cache_shape)
        flags = jnp.stack([me % 2, me // 2]).astype(jnp.int32)
        q_rot = q_proj(normed, w_q, cosine, sine)
        last = q_rot
        acts, attns, pieces = [], [], []
        for kind, first, rows, *place in SCHEDULE:
            if kind == 'mlp':
                normed, last = lax.optimization_barrier((normed, last))
                last = gate_up(normed, w_gate, w_up, first, rows, *place)
                acts.append((first, rows, last))
            if kind == 'own':
                q_rot, last = lax.optimization_barrier((q_rot, last))
                sources = (kv_own, kv_a, kv_b, kv_c)
                last = attend(flags, q_rot, first, rows, groups, sources, (1, 2), *place)
                attns.append((first, last))
            if kind == 'down':
                col, cols = place
                act = [(array, first - start) for start, many, array in acts if start <= first < start + many]
                attn = [array for start, array in attns if first <= start < first + rows]
                attn, last = lax.optimization_barrier((attn, last))
                last = down(act, attn, w_down, w_o, rows, col, cols)
                other = lax.ppermute(last, 'tp', [(0, 1), (1, 0)])
                pieces.append((last, other, first, col))
        hidden_out = None
        for part, other, first, col in pieces:
            hidden_out = add_chunk(hidden, part, other, hidden_out, first, col)
        return hidden_out, k_cache, v_cache

    row_spec = P(('dp', 'cp'), None)
    col_spec = P(None, 'tp')
    cache_spec = P(('dp', 'cp'), 'tp', None)
    in_specs = (row_spec, P(('dp', 'cp')), P(None), col_spec, col_spec, col_spec, P('tp', None), col_spec, col_spec, P('tp', None))
    return jax.shard_map(local_layer, mesh=mesh, in_specs=in_specs, out_specs=(row_spec, cache_spec, cache_spec), check_vma=False)
```

```python
import functools

import jax
import jax.numpy as jnp
from jax import lax
from jax.experimental import pallas as pl
from jax.experimental.pallas import tpu as pltpu
from jax.sharding import PartitionSpec as P


HEAD_DIM = 128
ROPE_BASE = 4000000
LN_EPS = 1e-5
LOG2E = 1.4426950408889634
BF16 = jnp.bfloat16
F32 = jnp.float32


def cost(flops, bytes_accessed, transcendentals=0):
    return pl.CostEstimate(flops=int(flops), bytes_accessed=int(bytes_accessed), transcendentals=int(transcendentals))


def rotary_tables(positions):
    lane = jnp.arange(HEAD_DIM)
    exponent = ((lane // 2) * 2).astype(F32) / HEAD_DIM
    inv_freq = 1.0 / (ROPE_BASE ** exponent)
    angles = positions.astype(F32)[:, None] * inv_freq[None, :]
    sign = jnp.where(lane % 2 == 0, -1.0, 1.0).astype(F32)
    return jnp.cos(angles), jnp.sin(angles) * sign[None, :]


def rotate_head(head, cosine, sine):
    even = lax.broadcasted_iota(jnp.int32, head.shape, 1) % 2 == 0
    other = jnp.where(even, pltpu.roll(head, HEAD_DIM - 1, 1), pltpu.roll(head, 1, 1))
    return (head * cosine + other * sine).astype(BF16)


def norm_kv_kernel(x_ref, gain_ref, wk_ref, wv_ref, cos_ref, sin_ref, h_ref, kv_ref, k_ref, v_ref):
    x = x_ref[...].astype(F32)
    width = x.shape[1]
    mean = jnp.sum(x, axis=1, keepdims=True) * (1.0 / width)
    centered = x - mean
    var = jnp.sum(centered * centered, axis=1, keepdims=True) * (1.0 / width)
    h_ref[...] = (centered * lax.rsqrt(var + LN_EPS) * gain_ref[...].astype(F32)[None, :]).astype(BF16)
    k = jnp.dot(h_ref[...], wk_ref[...], preferred_element_type=F32).astype(BF16)
    v = jnp.dot(h_ref[...], wv_ref[...], preferred_element_type=F32).astype(BF16)
    v_ref[...] = v
    cosine, sine = cos_ref[...], sin_ref[...]
    for head in range(k.shape[1] // HEAD_DIM):
        cols = slice(head * HEAD_DIM, (head + 1) * HEAD_DIM)
        rotated = rotate_head(k[:, cols].astype(F32), cosine, sine)
        k_ref[:, cols] = rotated
        kv_ref[head, 0] = rotated
        for start in range(0, k.shape[0], HEAD_DIM):
            kv_ref[head, 1, start:start + HEAD_DIM, :] = v[start:start + HEAD_DIM, cols].T


def norm_kv(x, gain, wk, wv, cosine, sine):
    rows, width = x.shape
    kv = wk.shape[1]
    groups = kv // HEAD_DIM
    tile = 256
    return pl.pallas_call(
        norm_kv_kernel,
        grid=(rows // tile,),
        in_specs=[
            pl.BlockSpec((tile, width), lambda i: (i, 0)),
            pl.BlockSpec((width,), lambda i: (0,)),
            pl.BlockSpec((width, kv), lambda i: (0, 0)),
            pl.BlockSpec((width, kv), lambda i: (0, 0)),
            pl.BlockSpec((tile, HEAD_DIM), lambda i: (i, 0)),
            pl.BlockSpec((tile, HEAD_DIM), lambda i: (i, 0)),
        ],
        out_specs=[
            pl.BlockSpec((tile, width), lambda i: (i, 0)),
            pl.BlockSpec((groups, 2, tile, HEAD_DIM), lambda i: (0, 0, i, 0)),
            pl.BlockSpec((tile, kv), lambda i: (i, 0)),
            pl.BlockSpec((tile, kv), lambda i: (i, 0)),
        ],
        out_shape=[
            jax.ShapeDtypeStruct((rows, width), BF16),
            jax.ShapeDtypeStruct((groups, 2, rows, HEAD_DIM), BF16),
            jax.ShapeDtypeStruct((rows, kv), BF16),
            jax.ShapeDtypeStruct((rows, kv), BF16),
        ],
        cost_estimate=cost(4 * rows * width * kv, 4 * rows * width + 4 * width * kv),
        name='norm_kv',
    )(x, gain, wk, wv, cosine, sine)


def q_kernel(h_ref, w_ref, cos_ref, sin_ref, q_ref):
    for start in range(0, h_ref.shape[0], 512):
        rows = slice(start, start + 512)
        q = jnp.dot(h_ref[rows, :], w_ref[...], preferred_element_type=F32).astype(BF16)
        cosine, sine = cos_ref[rows, :], sin_ref[rows, :]
        for head in range(q.shape[1] // HEAD_DIM):
            cols = slice(head * HEAD_DIM, (head + 1) * HEAD_DIM)
            q_ref[rows, cols] = rotate_head(q[:, cols].astype(F32), cosine, sine)


def q_proj(h, wq, cosine, sine):
    rows, width = h.shape
    cols = wq.shape[1]
    tile = 512
    return pl.pallas_call(
        q_kernel,
        grid=(cols // tile,),
        in_specs=[
            pl.BlockSpec((rows, width), lambda i: (0, 0)),
            pl.BlockSpec((width, tile), lambda i: (0, i)),
            pl.BlockSpec((rows, HEAD_DIM), lambda i: (0, 0)),
            pl.BlockSpec((rows, HEAD_DIM), lambda i: (0, 0)),
        ],
        out_specs=pl.BlockSpec((rows, tile), lambda i: (0, i)),
        out_shape=jax.ShapeDtypeStruct((rows, cols), BF16),
        cost_estimate=cost(2 * rows * width * cols, 2 * rows * width + 2 * width * cols),
        name='q_proj',
    )(h, wq, cosine, sine)


def attend_kernel(base, tile, chunk, group, blocks, columns, flags_ref, q_ref, *refs):
    sources = refs[:1 + sum(blocks)]
    o_ref, *out_refs, m_ref, l_ref, acc_ref, s0_ref, s1_ref = refs[1 + sum(blocks) + (1 + 2 * len(columns) if columns else 0):]
    if columns:
        x_ref, *halves = refs[1 + sum(blocks):][:1 + 2 * len(columns)]
        for n, col in enumerate(columns):
            mine_ref, other_ref = halves[2 * n:2 * n + 2]
            place = slice(col, col + mine_ref.shape[1])
            total = mine_ref[...].astype(F32) + other_ref[...].astype(F32)
            out_refs[0][:, place] = (x_ref[:, place].astype(F32) + total).astype(BF16)
    scale2 = (HEAD_DIM ** -0.5) * LOG2E
    step = pl.program_id(1)

    def scores(kv, keys, j, buffer, masked):
        q = q_ref[:, j * HEAD_DIM:(j + 1) * HEAD_DIM]
        top = None
        for start in range(0, keys, chunk):
            size = min(chunk, keys - start)
            s = lax.dot_general(kv[0, start:start + size, :], q, (((1,), (1,)), ((), ())), preferred_element_type=F32)
            if masked and start + size > keys - tile:
                key = lax.broadcasted_iota(jnp.int32, s.shape, 0) + start
                query = lax.broadcasted_iota(jnp.int32, s.shape, 1) + (keys - tile)
                s = jnp.where(key <= query, s, -jnp.inf)
            buffer[start:start + size, :] = s
            part = jnp.max(s.reshape(size // 8, 8, tile), axis=0)
            top = part if top is None else jnp.maximum(top, part)
        return top

    def block(full, keys, first, masked):
        items = [(kv, j) for kv in full for j in range(group)]
        buffers = (s0_ref, s1_ref)
        top8 = scores(items[0][0], keys, items[0][1], buffers[0], masked)
        for n, (kv, j) in enumerate(items):
            top = jnp.max(top8, axis=0, keepdims=True)
            if not first:
                old = m_ref[j]
                top = jnp.maximum(top, old)
            if n + 1 < len(items):
                top8 = scores(items[n + 1][0], keys, items[n + 1][1], buffers[(n + 1) % 2], masked)
            total = part = None
            for start in range(0, keys, chunk):
                size = min(chunk, keys - start)
                e = jnp.exp2((buffers[n % 2][start:start + size, :] - top) * scale2)
                e8 = jnp.sum(e.reshape(size // 8, 8, tile), axis=0)
                vt = jnp.concatenate([kv[1, at:at + HEAD_DIM, :] for at in range(start, start + size, HEAD_DIM)], axis=1)
                product = lax.dot_general(vt, e.astype(BF16), (((1,), (0,)), ((), ())), preferred_element_type=F32)
                total = e8 if total is None else total + e8
                part = product if part is None else part + product
            total = jnp.sum(total, axis=0, keepdims=True)
            if not first:
                factor = jnp.exp2((old - top) * scale2)
                total = total + l_ref[j] * factor
                part = part + acc_ref[j] * factor
            m_ref[j] = top
            l_ref[j] = total
            acc_ref[j] = part

    for n in range(pl.num_programs(1)):

        @pl.when(step == n)
        def _():
            block(sources[:1], base + (n + 1) * tile, True, True)

    start = 1
    for flag, many in enumerate(blocks):
        full = sources[start:start + many]
        start += many

        @pl.when(flags_ref[flag] > 0)
        def _():
            block(full, full[0].shape[1], False, False)

    for j in range(group):
        out = acc_ref[j] / l_ref[j]
        o_ref[:, j * HEAD_DIM:(j + 1) * HEAD_DIM] = out.T.astype(BF16)


def attend(flags, q, base, count, groups, sources, blocks, tile, x=None, pieces=()):
    keys = sources[0].shape[2]
    width = q.shape[1] // groups
    group = width // HEAD_DIM
    first = base // tile

    kv_spec = pl.BlockSpec((None, 2, keys, HEAD_DIM), lambda g, i, f: (g, 0, 0, 0))
    steps = count // tile
    extra = [x] + [array for mine, other, _, _ in pieces for array in (mine, other)] if pieces else []
    share = pieces[0][0].shape[0] // (groups * steps) if pieces else 0
    extra_specs = [pl.BlockSpec((share, array.shape[1]), lambda g, i, f: (g * steps + i, 0)) for array in extra]
    grid_spec = pltpu.PrefetchScalarGridSpec(
        num_scalar_prefetch=1,
        grid=(groups, count // tile),
        in_specs=[pl.BlockSpec((tile, width), lambda g, i, f: (first + i, g))] + [kv_spec] * len(sources) + extra_specs,
        out_specs=[pl.BlockSpec((tile, width), lambda g, i, f: (i, g))] + extra_specs[:1],
        scratch_shapes=[
            pltpu.VMEM((group, 1, tile), F32),
            pltpu.VMEM((group, 1, tile), F32),
            pltpu.VMEM((group, HEAD_DIM, tile), F32),
            pltpu.VMEM((keys, tile), F32),
            pltpu.VMEM((keys, tile), F32),
        ],
    )
    return pl.pallas_call(
        functools.partial(attend_kernel, base, tile, 512, group, blocks, tuple(col for _, _, _, col in pieces)),
        grid_spec=grid_spec,
        out_shape=[jax.ShapeDtypeStruct((count, q.shape[1]), BF16)] + ([jax.ShapeDtypeStruct(x.shape, BF16)] if pieces else []),
        cost_estimate=cost(10 * count * keys * q.shape[1], 4 * len(sources) * keys * groups * HEAD_DIM, 3 * count * keys * groups * group),
        name='attend',
    )(flags, q, *sources, *extra)


def gate_up_kernel(h_ref, wg_ref, wu_ref, a_ref):
    gate = jnp.dot(h_ref[...], wg_ref[...], preferred_element_type=F32).astype(BF16).astype(F32)
    up = jnp.dot(h_ref[...], wu_ref[...], preferred_element_type=F32).astype(BF16).astype(F32)
    a_ref[...] = (gate * jax.nn.sigmoid(gate) * up).astype(BF16)


def gate_up(h, wg, wu, first, rows, col, cols):
    width = wg.shape[0]
    tile = 512
    index, start = first // rows, col // tile
    weight_spec = pl.BlockSpec((width, tile), lambda i: (0, start + i))
    return pl.pallas_call(
        gate_up_kernel,
        grid=(cols // tile,),
        in_specs=[pl.BlockSpec((rows, width), lambda i: (index, 0)), weight_spec, weight_spec],
        out_specs=pl.BlockSpec((rows, tile), lambda i: (0, i)),
        out_shape=jax.ShapeDtypeStruct((rows, cols), BF16),
        cost_estimate=cost(4 * rows * width * cols, 2 * rows * (width + cols) + 4 * width * cols),
        name='gate_up',
    )(h, wg, wu)


def down_kernel(acts, attns, streams, *refs):
    a_refs, o_refs = refs[:acts], refs[acts:acts + attns]
    w_refs, wo_ref, out_ref = refs[acts + attns:acts + attns + streams], refs[-2], refs[-1]
    depth = w_refs[0].shape[0]
    rows = out_ref.shape[0] // attns
    a_parts = [a_ref.at[:, start:start + depth] for a_ref in a_refs for start in range(0, a_ref.shape[1], depth)]
    for n, o_ref in enumerate(o_refs):
        place = slice(n * rows, (n + 1) * rows)
        total = jnp.dot(o_ref[...], wo_ref[...], preferred_element_type=F32)
        for a_part, w_ref in zip(a_parts, w_refs):
            total += jnp.dot(a_part[place, :], w_ref[...], preferred_element_type=F32)
        out_ref[place, :] = total.astype(BF16)


def down(acts, attns, wd, wo, rows, col, cols):
    tile = 512
    start = col // tile
    streams = 1
    depth = wd.shape[0] // streams

    def act_spec(array, row):
        return pl.BlockSpec((rows, array.shape[1]), lambda i: (row // rows, 0))

    def stream_spec(n):
        return pl.BlockSpec((depth, tile), lambda i: (n, start + i))

    return pl.pallas_call(
        functools.partial(down_kernel, len(acts), len(attns), streams),
        grid=(cols // tile,),
        in_specs=[act_spec(*pair) for pair in acts]
        + [pl.BlockSpec(o.shape, lambda i: (0, 0)) for o in attns]
        + [stream_spec(n) for n in range(streams)]
        + [pl.BlockSpec((wo.shape[0], tile), lambda i: (0, start + i))],
        out_specs=pl.BlockSpec((rows, tile), lambda i: (0, i)),
        out_shape=jax.ShapeDtypeStruct((rows, cols), BF16),
        cost_estimate=cost(2 * rows * (wd.shape[0] + wo.shape[0]) * cols, 2 * cols * (wd.shape[0] + wo.shape[0])),
        name='down',
    )(*[array for array, _ in acts], *attns, *[wd] * streams, wo)


def add_kernel(x_ref, mine_ref, other_ref, *refs):
    total = mine_ref[...].astype(F32) + other_ref[...].astype(F32)
    refs[-1][...] = (x_ref[...].astype(F32) + total).astype(BF16)


def add_chunk(x, mine, other, out, first, col):
    rows, cols = mine.shape
    tile = 128 if rows * cols == 256 * 3072 else 256
    index, start = first // tile, col // cols
    place = pl.BlockSpec((tile, cols), lambda i: (index + i, start))
    chunk = pl.BlockSpec((tile, cols), lambda i: (i, 0))
    args, specs, alias = [x, mine, other], [place, chunk, chunk], {}
    if out is not None:
        args, specs, alias = args + [out], specs + [pl.BlockSpec(memory_space=pl.ANY)], {3: 0}
    return pl.pallas_call(
        add_kernel,
        grid=(rows // tile,),
        in_specs=specs,
        out_specs=place,
        out_shape=jax.ShapeDtypeStruct(x.shape, BF16),
        input_output_aliases=alias,
        cost_estimate=cost(3 * rows * cols, 8 * rows * cols),
        name='add',
    )(*args)


SCHEDULE = (
    ('mlp', 0, 512, 0, 4096),
    ('own', 0, 512, 512),
    ('down', 0, 512, 2560, 512),
    ('down', 0, 512, 0, 2560),
    ('mlp', 512, 512, 0, 4096),
    ('own', 512, 256, 256),
    ('down', 512, 256, 0, 3072),
    ('own', 768, 256, 256, 2),
    ('down', 768, 256, 0, 2048),
    ('down', 768, 256, 2048, 1024),
)


def solution(mesh):
    if mesh.shape['cp'] != 4 or mesh.shape['tp'] != 2:
        raise ValueError('mesh')

    def local_layer(hidden, positions, ln_gain, w_q, w_k, w_v, w_o, w_gate, w_up, w_down):
        me = lax.axis_index('cp')
        cosine, sine = rotary_tables(positions)
        normed, kv_own, k_own, v_own = norm_kv(hidden, ln_gain, w_k, w_v, cosine, sine)
        groups = kv_own.shape[0]
        send = functools.partial(lax.ppermute, axis_name='cp')
        kv_b = send(kv_own, perm=[(0, 2), (1, 3)])
        kv_a = send(kv_own, perm=[(0, 1), (2, 3)])
        kv_c = send(kv_b, perm=[(2, 3), (3, 2)])
        cache_shape = (k_own.shape[0], groups, HEAD_DIM)
        k_cache, v_cache = k_own.reshape(cache_shape), v_own.reshape(cache_shape)
        flags = jnp.stack([me % 2, me // 2]).astype(jnp.int32)
        q_rot = q_proj(normed, w_q, cosine, sine)
        last = q_rot
        acts, attns, pieces, hidden_out = [], [], [], None
        for kind, first, rows, *place in SCHEDULE:
            if kind == 'mlp':
                normed, last = lax.optimization_barrier((normed, last))
                last = gate_up(normed, w_gate, w_up, first, rows, *place)
                acts.append((first, rows, last))
            if kind == 'own':
                q_rot, last = lax.optimization_barrier((q_rot, last))
                sources = (kv_own, kv_a, kv_b, kv_c)
                tile, *merged = place
                added = pieces[:merged[0]] if merged else []
                last, *outs = attend(flags, q_rot, first, rows, groups, sources, (1, 2), tile, hidden, added)
                if merged:
                    (hidden_out,), pieces = outs, pieces[merged[0]:]
                attns.append((first, last))
            if kind == 'down':
                col, cols = place
                act = [(array, first - start) for start, many, array in acts if start <= first < start + many]
                attn = [array for start, array in attns if first <= start < first + rows]
                attn, last = lax.optimization_barrier((attn, last))
                last = down(act, attn, w_down, w_o, rows, col, cols)
                other = lax.ppermute(last, 'tp', [(0, 1), (1, 0)])
                pieces.append((last, other, first, col))
        for part, other, first, col in pieces:
            hidden_out = add_chunk(hidden, part, other, hidden_out, first, col)
        return hidden_out, k_cache, v_cache

    row_spec = P(('dp', 'cp'), None)
    col_spec = P(None, 'tp')
    cache_spec = P(('dp', 'cp'), 'tp', None)
    in_specs = (row_spec, P(('dp', 'cp')), P(None), col_spec, col_spec, col_spec, P('tp', None), col_spec, col_spec, P('tp', None))
    return jax.shard_map(local_layer, mesh=mesh, in_specs=in_specs, out_specs=(row_spec, cache_spec, cache_spec), check_vma=False)
```
